32 devices in a mesh: dp: 2 (over x), tp: 16 (over y, z, core).
Axes of the slice: x: 2, y: 2, z: 4, core: 2. Of those that a mesh axis runs over, the one named last changes fastest.
Arguments:
- x: bfloat16 [4096, 16384], P('dp'), parts along dimension 0
- gain: bfloat16 [16384], replicated
- wq: bfloat16 [16384, 16384], P(None, 'tp')
- wk: bfloat16 [16384, 16384], P(None, 'tp')
- wv: bfloat16 [16384, 16384], P(None, 'tp')
- wo: bfloat16 [16384, 16384], P('tp')
Outputs:
- output: bfloat16 [4096, 16384], P('dp'), parts along dimension 0
There are 2 independent parts. The reference program is written for one: setup_inputs(seed, part) draws one part's arguments, and reference() takes and returns one part's arrays. A program takes and returns all parts, laid end to end along the dimension named above; an argument that names none is the same for every part.
All inputs are finite; a program needn't handle non-finite values.
Results may differ from the reference program's by a relative error of at most 0.012.
Values are sent between devices in bfloat16 or wider.
A program may use at most 2 GiB of HBM per device.

```python
import jax
import jax.numpy as jnp
from jax import lax

ROWS = 2048
D = 16384
HEADS = 128
KV_HEADS = 128
HEAD = 128
THETA = 10000


def setup_inputs(seed: int = 0, part: int = 0) -> dict:
    kx, kn, kq, kk, kv, ko = jax.random.split(jax.random.key(seed), 6)

    def weights(key, rows, columns):
        return jax.random.normal(key, (rows, columns), jnp.float32) * rows**-0.5

    drawn = {
        "x": jax.random.normal(jax.random.fold_in(kx, part), (ROWS, D), jnp.float32),
        "gain": 1 + 0.1 * jax.random.normal(kn, (D,), jnp.float32),
        "wq": 2 * weights(kq, D, HEADS * HEAD),
        "wk": 2 * weights(kk, D, KV_HEADS * HEAD),
        "wv": 4 * weights(kv, D, KV_HEADS * HEAD),
        "wo": weights(ko, HEADS * HEAD, D),
    }
    return {k: v.astype(jnp.bfloat16) for k, v in drawn.items()}


def normed(x, gain):
    wide = x.astype(jnp.float32)
    scale = lax.rsqrt(jnp.mean(wide * wide, -1, keepdims=True) + 1e-6)
    return (wide * scale * gain.astype(jnp.float32)).astype(jnp.bfloat16)


def turned(t, place, theta):
    half = t.shape[-1] // 2
    angle = place.astype(jnp.float32)[:, None] * theta ** (-jnp.arange(half, dtype=jnp.float32) / half)
    cos, sin = jnp.cos(angle)[:, None], jnp.sin(angle)[:, None]
    a, b = t[..., :half].astype(jnp.float32), t[..., half:].astype(jnp.float32)
    return jnp.concatenate([a * cos - b * sin, b * cos + a * sin], -1).astype(jnp.bfloat16)


def matmul(a, w):
    return jnp.dot(a, w, preferred_element_type=jnp.float32).astype(jnp.bfloat16)


def einsum(form, a, b):
    return jnp.einsum(form, a.astype(jnp.float32), b.astype(jnp.float32))


def attention(q, k, v):
    scores = einsum("tgsd,ugd->gstu", q, k) * q.shape[-1] ** -0.5
    token = jnp.arange(q.shape[0])
    scores = jnp.where(token[:, None] >= token, scores, -jnp.inf)
    weights = jax.nn.softmax(scores, -1).astype(jnp.bfloat16)
    return einsum("gstu,ugd->tgsd", weights, v).astype(jnp.bfloat16)


def reference(x, gain, wq, wk, wv, wo):
    a, place = normed(x, gain), jnp.arange(ROWS)
    q = turned(matmul(a, wq).reshape(ROWS, HEADS, HEAD), place, THETA).reshape(ROWS, KV_HEADS, -1, HEAD)
    k = turned(matmul(a, wk).reshape(ROWS, KV_HEADS, HEAD), place, THETA)
    v = matmul(a, wv).reshape(ROWS, KV_HEADS, HEAD)
    seen = attention(q, k, v).reshape(ROWS, HEADS * HEAD)
    return (x.astype(jnp.float32) + jnp.dot(seen, wo, preferred_element_type=jnp.float32)).astype(jnp.bfloat16)
```

```python
import functools

import jax
import jax.numpy as jnp
from jax import lax
from jax.experimental import pallas as pl
from jax.experimental.pallas import tpu as pltpu
from jax.sharding import PartitionSpec as P

HEAD = 128
THETA = 10000
NEG = -1e30
LOG2E = 1.4426950408889634
MESH = pl.DeviceIdType.MESH

ROWS = 2048
D = 16384
MINE = 1024
PAIR = 2 * MINE
HALF = 8192
W1, W2, WB = 1152, 896, 256
WA = W1 - WB
CH = 256
SUB = 16
PER = CH // SUB
NCH = ROWS // CH
NSUB = ROWS // SUB
KEEP = 4
KS, TN = 4096, 512
NS = 3
TALL, WIDE = 16, 2048
QT, QK = 3 * 1024 // TN, D // KS
UQ = QT * QK
UO = HALF // (2 * TN)
UNITS = UQ + UO
KINDS = (BB, Y1, E2, E1, X2, X1, Y2, FP, FX, FY, AP, AY, CP, CX, EY0, EY1, SIB, SEEN, WO) = range(19)
LAG = 2
STAGES = 8
QKV, ATT, OUT = 1, 11, 13


def _dot(a, b, ca, cb):
    return lax.dot_general(a, b, (((ca,), (cb,)), ((), ())), preferred_element_type=jnp.float32)


def kernel(x, gain, freq, wq, wk, wv, wo, y, wos,
           a, w, acc, csv, gain8, q_s, k_s, v_s, seen, top_s, mix_s, term,
           bb, be2, be1, sy1, ry1, sx2, rx2, sx1, rx1, sy2, ry2, fin, res,
           ssem, rsem, wsem, lsem, rssem, xsem, credit, *, compute, comm):
    t = lax.axis_index("tp")
    yy, z, core = t // 8, lax.rem(t // 2, 4), lax.rem(t, 2)
    mid = (z == 1) | (z == 2)
    end = jnp.logical_not(mid)
    s = z // 2
    yo, so = 1 - yy, 1 - s
    to_y = yo * 8 + z * 2 + core
    to_p = yy * 8 + (z + 1 - 2 * lax.rem(z, 2)) * 2 + core
    to_x = yy * 8 + jnp.where(mid, 3 - z, z) * 2 + core
    to_s = yy * 8 + z * 2 + 1 - core

    def greet(act):
        for n, dev in enumerate((to_y, to_p, to_s)):
            act(n, dev)

        @pl.when(mid)
        def _():
            act(3, to_x)

    def signal(sem, dev):
        pl.semaphore_signal(sem, inc=1, device_id={"tp": dev}, device_id_type=MESH)

    bar = pltpu.get_barrier_semaphore()
    greet(lambda n, dev: signal(bar, dev))

    @pl.when(mid)
    def _():
        pl.semaphore_wait(bar, 4)

    @pl.when(end)
    def _():
        pl.semaphore_wait(bar, 3)

    def rc(kind, slot, src, dst, dev):
        return pltpu.make_async_remote_copy(src_ref=src, dst_ref=dst, send_sem=ssem.at[kind, slot], recv_sem=rsem.at[kind, slot],
                                            device_id={"tp": dev}, device_id_type=MESH)

    def cols(at, n):
        return pl.ds(pl.multiple_of(at, 128), n)

    mine, other = core * HALF, (1 - core) * HALF

    def t1(r, p):
        return (2 * r + p) * (W1 + W2)

    def t2(r, p):
        return t1(r, p) + W1

    def exchange(m):
        def stage(n, who=None):
            o = LAG * n
            ok = (m >= o) & (m < NSUB + o)
            return lambda body: pl.when(ok if who is None else ok & who)(functools.partial(body, Stage(m - o)))

        class Stage:
            def __init__(self, j):
                self.j, self.slot = j, lax.rem(j, KEEP)
                self.rows = pl.ds(pl.multiple_of(j * SUB, SUB), SUB)

            def y(self, at, n, first=mine):
                return y.at[self.rows, cols(first + at, n)]

            def term(self, at, n):
                rows = pl.ds(pl.multiple_of(lax.rem(self.j, PER) * SUB, SUB), SUB)
                return term.at[lax.rem(self.j // PER, 2), rows, cols(at, n)]

            def buf(self, ref, at=0, n=None):
                return ref.at[self.slot, :, cols(at, ref.shape[-1] if n is None else n)]

            def wide(self, ref, at=0, n=None):
                return self.buf(ref, at, n)[...].astype(jnp.float32)

            def copy(self, kind, src, dst=None, dev=to_y):
                return rc(kind, self.slot, src, src if dst is None else dst, dev)

            def send(self, kind, dev, src, dst=None):
                self.copy(kind, src, dst, dev).start()

            def got(self, kind, ref):
                self.copy(kind, ref).wait_recv()

            def gone(self, kind, ref):
                self.copy(kind, ref).wait_send()

            def residual(self):
                return pltpu.make_async_copy(x.at[self.rows, cols(mine + t1(yy, s), W1 + W2)], self.buf(res), rssem.at[self.slot])

            def keep(self):
                return pltpu.make_async_copy(self.buf(fin), self.y(t1(yy, s), W1 + W2), lsem.at[self.slot])

        low = jnp.bfloat16

        def grow(e, at, n, more):
            own = e.term(at, n)
            own[...] = own[...] + more

        @stage(0, mid)
        def _(e):
            for p in range(2):
                e.buf(bb, p * WB, WB)[...] = e.term(t1(yo, p) + WA, WB)[...].astype(low)

        @stage(1, mid)
        def _(e):
            e.gone(BB, e.buf(bb))
            for p in range(2):
                e.buf(sy1, p * WA, WA)[...] = e.term(t1(yo, p), WA)[...].astype(low)

        @stage(1, end)
        def _(e):
            e.got(BB, e.buf(bb))
            for p in range(2):
                e.buf(sy1, p * W1, WA)[...] = e.term(t1(yo, p), WA)[...].astype(low)
                e.buf(sy1, p * W1 + WA, WB)[...] = (e.term(t1(yo, p) + WA, WB)[...] + e.wide(bb, p * WB, WB)).astype(low)
            for q in range(4):
                e.buf(be2, q * W2, W2)[...] = e.term(t2(0, q), W2)[...].astype(low)

        @stage(2, mid)
        def _(e):
            e.gone(Y1, e.buf(sy1, 0, 2 * WA))
            e.got(Y1, e.buf(ry1, 0, 2 * WA))
            e.got(E2, e.buf(be2))
            for p in range(2):
                grow(e, t1(yy, p), WA, e.wide(ry1, p * WA, WA))
            for r in range(2):
                e.buf(sx2, r * W2, W2)[...] = (e.term(t2(r, so), W2)[...] + e.wide(be2, (2 * r + so) * W2, W2)).astype(low)
                grow(e, t2(r, s), W2, e.wide(be2, (2 * r + s) * W2, W2))

        @stage(2, end)
        def _(e):
            e.gone(Y1, e.buf(sy1))
            e.got(Y1, e.buf(ry1))
            e.gone(E2, e.buf(be2))
            for p in range(2):
                e.buf(be1, p * W1, W1)[...] = (e.term(t1(yy, p), W1)[...] + e.wide(ry1, p * W1, W1)).astype(low)

        @stage(3, end)
        def _(e):
            e.gone(E1, e.buf(be1))

        @stage(3, mid)
        def _(e):
            e.gone(X2, e.buf(sx2))
            e.got(E1, e.buf(be1))
            e.buf(sx1)[...] = (e.term(t1(yy, so), W1)[...] + e.wide(be1, so * W1, W1)).astype(low)
            grow(e, t1(yy, s), W1, e.wide(be1, s * W1, W1))
            e.got(X2, e.buf(rx2))
            e.buf(sy2)[...] = (e.term(t2(yo, s), W2)[...] + e.wide(rx2, yo * W2, W2)).astype(low)
            grow(e, t2(yy, s), W2, e.wide(rx2, yy * W2, W2))

        @stage(4, mid)
        def _(e):
            e.gone(X1, e.buf(sx1))
            e.gone(Y2, e.buf(sy2))
            e.residual().wait()
            e.got(X1, e.buf(rx1))
            e.got(Y2, e.buf(ry2))
            for at, n, ref in ((0, W1, rx1), (W1, W2, ry2)):
                e.buf(fin, at, n)[...] = (e.term(t1(yy, s) + at, n)[...] + e.wide(ref) + e.wide(res, at, n)).astype(low)

        @stage(5, mid)
        def _(e):
            for kind in (FP, FX, FY):
                e.gone(kind, e.buf(fin))
            e.keep().wait()
            e.got(FX, e.y(t1(yy, so), W1 + W2))
            e.got(FY, e.y(t1(yo, s), W1 + W2))

        @stage(5, end)
        def _(e):
            e.got(FP, e.y(t1(yy, s), W1 + W2))

        @stage(6, mid)
        def _(e):
            e.gone(AP, e.y(0, W1 + W2))
            e.gone(AY, e.y(0, W1))
            e.gone(CP, e.y(0, W2))
            e.gone(CX, e.y(0, W2))
            e.got(AY, e.y(t1(yo, so), W1))
            e.got(CX, e.y(t2(yo, so), W2))

        @stage(6, end)
        def _(e):
            e.gone(EY0, e.y(0, W1))
            e.got(AP, e.y(t1(yy, so), W1 + W2))
            e.got(CP, e.y(t2(yo, s), W2))
            e.got(EY0, e.y(t1(yo, s), W1))

        @stage(7, end)
        def _(e):
            e.gone(EY1, e.y(0, W1 + W2))
            e.got(EY1, e.y(t1(yo, so), W1 + W2))

        @stage(8)
        def _(e):
            e.gone(SIB, e.y(0, HALF))
            e.got(SIB, e.y(0, HALF, other))

        @pl.when(m >= LAG)
        def _():
            greet(lambda n, dev: pl.semaphore_wait(credit.at[n], 1))

        @stage(0, mid)
        def _(e):
            e.send(BB, to_p, e.buf(bb))

        @stage(1, end)
        def _(e):
            e.send(Y1, to_y, e.buf(sy1), e.buf(ry1))
            e.send(E2, to_p, e.buf(be2))

        @stage(1, mid)
        def _(e):
            e.send(Y1, to_y, e.buf(sy1, 0, 2 * WA), e.buf(ry1, 0, 2 * WA))

        @stage(2, end)
        def _(e):
            e.send(E1, to_p, e.buf(be1))

        @stage(2, mid)
        def _(e):
            e.send(X2, to_x, e.buf(sx2), e.buf(rx2))

        @stage(3, mid)
        def _(e):
            e.send(X1, to_x, e.buf(sx1), e.buf(rx1))
            e.send(Y2, to_y, e.buf(sy2), e.buf(ry2))
            e.residual().start()

        @stage(4, mid)
        def _(e):
            for kind, dev in ((FP, to_p), (FX, to_x), (FY, to_y)):
                e.send(kind, dev, e.buf(fin), e.y(t1(yy, s), W1 + W2))
            e.keep().start()

        @stage(5, mid)
        def _(e):
            e.send(AP, to_p, e.y(t1(yy, so), W1 + W2))
            e.send(CX, to_x, e.y(t2(yo, s), W2))
            e.send(AY, to_y, e.y(t1(yy, so), W1))
            e.send(CP, to_p, e.y(t2(yo, s), W2))

        @stage(5, end)
        def _(e):
            e.send(EY0, to_y, e.y(t1(yy, s), W1))

        @stage(6, end)
        def _(e):
            e.send(EY1, to_y, e.y(t1(yy, so), W1 + W2))

        @stage(7)
        def _(e):
            e.send(SIB, to_s, e.y(0, HALF))

        greet(lambda n, dev: signal(credit.at[n], dev))

    wo_sent = rc(WO, 0, wo.at[:, cols(other, HALF)], wos, to_s)

    def tiles(g):
        u, k = lax.rem(g, UNITS), lax.rem(g, NS)

        def proj(ref, n):
            @pl.when((u >= n * (UQ // 3)) & (u < (n + 1) * (UQ // 3)))
            def _():
                v = u - n * (UQ // 3)
                pltpu.make_async_copy(ref.at[pl.ds(pl.multiple_of(lax.rem(v, QK) * KS, KS), KS), cols(v // QK * TN, TN)], w.at[k], wsem.at[k]).start()

        @pl.when(g < NCH * UNITS)
        def _():
            for n, ref in enumerate((wq, wk, wv)):
                proj(ref, n)

            @pl.when(u >= UQ)
            def _():
                @pl.when(g == UQ)
                def _():
                    wo_sent.wait_recv()

                for n in range(2):
                    v = 2 * (u - UQ) + n
                    for ref, at, row in ((wo, mine, 0), (wos, 0, MINE)):
                        src = ref.at[:, cols(at + v * TN, TN)]
                        pltpu.make_async_copy(src, w.at[k, pl.ds(n * PAIR + row, MINE)], wsem.at[k]).start()

    def tile(g):
        k = lax.rem(g, NS)
        pltpu.make_async_copy(w.at[k], w.at[k], wsem.at[k]).wait()
        return w.at[k]

    def rows_of(c):
        return pl.ds(pl.multiple_of(c * CH, CH), CH)

    def fetch(c):
        return pltpu.make_async_copy(x.at[rows_of(c)], a, xsem)

    def angles(c):
        place = c * CH + lax.broadcasted_iota(jnp.int32, (CH, HEAD), 0)
        angle = place.astype(jnp.float32) * freq[...]
        first = lax.broadcasted_iota(jnp.int32, (CH, HEAD), 1) < HEAD // 2
        sin = jnp.sin(angle)
        csv[:, :HEAD] = jnp.cos(angle)
        csv[:, HEAD:] = jnp.where(first, -sin, sin)

    def norm():
        def group(r, _):
            rows = pl.ds(pl.multiple_of(r * TALL, TALL), TALL)
            total = jnp.zeros((TALL, HEAD), jnp.float32)
            for n in range(D // WIDE):
                wide = a[rows, n * WIDE:(n + 1) * WIDE].astype(jnp.float32)
                sq = wide * wide
                for i in range(WIDE // HEAD):
                    total = total + sq[:, i * HEAD:(i + 1) * HEAD]
            scale = lax.rsqrt(jnp.sum(total, -1, keepdims=True) * (1 / D) + 1e-6)
            for n in range(D // WIDE):
                at = slice(n * WIDE, (n + 1) * WIDE)
                a[rows, at] = (a[rows, at].astype(jnp.float32) * scale * jnp.concatenate([gain8[:, at]] * (TALL // 8))).astype(jnp.bfloat16)
            return None

        lax.fori_loop(0, CH // TALL, group, None)

    def turn(b):
        b = b.astype(jnp.float32)
        return (b * csv[:, :HEAD] + pltpu.roll(b, HEAD // 2, 1) * csv[:, HEAD:]).astype(jnp.bfloat16)

    def project(c, u, _):
        g = c * UNITS + u
        ref = tile(g)
        ks, n = lax.rem(u, QK), u // QK
        acc[...] += jnp.dot(a[:, cols(ks * KS, KS)], ref[...], preferred_element_type=jnp.float32)
        tiles(g + NS)

        @pl.when(ks == QK - 1)
        def _():
            heads = [(lax.rem(n, 2) * (TN // HEAD) + i, slice(i * HEAD, (i + 1) * HEAD)) for i in range(TN // HEAD)]

            @pl.when(n < 2)
            def _():
                for h, at in heads:
                    q_s[h] = turn(acc[:, at].astype(jnp.bfloat16))

            @pl.when((n >= 2) & (n < 4))
            def _():
                for h, at in heads:
                    k_s[h, rows_of(c), :] = turn(acc[:, at].astype(jnp.bfloat16))

            @pl.when(n >= 4)
            def _():
                for h, at in heads:
                    v_s[h, :, cols(c * CH, CH)] = acc[:, at].astype(jnp.bfloat16).T

            acc[...] = jnp.zeros_like(acc)
        return None

    def attend(c, h0, count):
        e = HEAD**-0.5 * LOG2E
        for i in range(count):
            top_s[i:i + 1, :] = jnp.full((1, CH), NEG, jnp.float32)
            mix_s[i] = jnp.zeros((HEAD + 8, CH), jnp.float32)
        ones = jnp.ones((8, CH), jnp.bfloat16)

        def block(j, masked):
            here = pl.ds(pl.multiple_of(j * CH, CH), CH)
            scores = [_dot(k_s[h0 + i, here, :], q_s[h0 + i], 1, 1) for i in range(count)]
            if masked:
                ok = lax.broadcasted_iota(jnp.int32, (CH, CH), 1) >= lax.broadcasted_iota(jnp.int32, (CH, CH), 0)
            weights, keeps = [], []
            for i, sc in enumerate(scores):
                if masked:
                    sc = jnp.where(ok, sc, 2 * NEG)
                old = top_s[i:i + 1, :]
                top = jnp.maximum(old, sc.max(axis=0, keepdims=True))
                top_s[i:i + 1, :] = top
                weights.append(jnp.exp2((sc - top) * e).astype(jnp.bfloat16))
                keeps.append(jnp.exp2((old - top) * e))
            for i, (p, kp) in enumerate(zip(weights, keeps)):
                values = jnp.concatenate([v_s[h0 + i, :, here], ones], axis=0)
                mix_s[i] = mix_s[i] * kp + _dot(values, p, 1, 0)

        lax.fori_loop(0, c, lambda j, _: block(j, False), None)
        block(c, True)
        for i in range(count):
            out = mix_s[i, :HEAD, :] * (1 / mix_s[i, HEAD:HEAD + 1, :])
            seen[:, cols((h0 + i) * HEAD, HEAD)] = out.T.astype(jnp.bfloat16)

    def out_tile(c, v, _):
        g = c * UNITS + UQ + v
        ref = tile(g)
        for n in range(2):
            part = jnp.dot(seen[...], ref[n * PAIR:(n + 1) * PAIR], preferred_element_type=jnp.float32)
            term[lax.rem(c, 2), :, cols((2 * v + n) * TN, TN)] = part
        tiles(g + NS)
        return None

    seen_sent = rc(SEEN, 0, seen.at[:, pl.ds(0, 1024)], seen.at[:, pl.ds(1024, 1024)], to_s)

    if compute:
        fetch(0).start()
        for g in range(NS):
            tiles(g)
        wo_sent.start()
        acc[...] = jnp.zeros_like(acc)
        gain8[...] = jnp.broadcast_to(gain[...].astype(jnp.float32), gain8.shape)

    def step(n, _):
        c, i = n // PER, lax.rem(n, PER)
        if compute:
            @pl.when((c < NCH) & (i == OUT))
            def _():
                seen_sent.start()

        if comm:
            @pl.when(c >= 1)
            def _():
                exchange((c - 1) * PER + i)

        def slot(first, last):
            return pl.when((c < NCH) & (i >= first) & (i < last))

        if compute:
            @slot(0, QKV)
            def _():
                angles(c)
                fetch(c).wait()
                norm()

            @slot(QKV, ATT)
            def _():
                lax.fori_loop((i - QKV) * UQ // (ATT - QKV), (i - QKV + 1) * UQ // (ATT - QKV), functools.partial(project, c), None)

            @slot(ATT, ATT + 1)
            def _():
                @pl.when(c < NCH - 1)
                def _():
                    fetch(c + 1).start()

            @slot(ATT, OUT)
            def _():
                attend(c, (i - ATT) * (8 // (OUT - ATT)), 8 // (OUT - ATT))

            @slot(OUT, OUT + 1)
            def _():
                seen_sent.wait_recv()
                seen_sent.wait_send()

            @slot(OUT, PER)
            def _():
                lax.fori_loop((i - OUT) * UO // (PER - OUT), (i - OUT + 1) * UO // (PER - OUT), functools.partial(out_tile, c), None)

        return None

    steps = NSUB + LAG * (STAGES + 1)
    lax.fori_loop(0, PER + (steps if comm else NSUB - PER), step, None)
    if comm:
        greet(lambda n, dev: pl.semaphore_wait(credit.at[n], LAG))
    if compute:
        wo_sent.wait_send()


def call(x, gain, freq, wq, wk, wv, wo, compute=True, comm=True, cid=0):
    any_, vmem = pl.BlockSpec(memory_space=pl.ANY), pl.BlockSpec(memory_space=pltpu.VMEM)
    low = jnp.bfloat16
    v, f32 = pltpu.VMEM, jnp.float32
    msg = lambda n: v((KEEP, SUB, n), low)
    return pl.pallas_call(
        functools.partial(kernel, compute=compute, comm=comm),
        out_shape=[jax.ShapeDtypeStruct((ROWS, D), low), jax.ShapeDtypeStruct((1024, HALF), low)],
        in_specs=[any_, vmem, vmem] + [any_] * 4,
        out_specs=[any_, any_],
        scratch_shapes=[
            v((CH, D), low), v((NS, KS, TN), low), v((CH, TN), f32), v((CH, 2 * HEAD), f32), v((8, D), f32),
            v((8, CH, HEAD), low), v((8, ROWS, HEAD), low), v((8, HEAD, ROWS), low), v((CH, 2048), low),
            v((8, CH), f32), v((4, HEAD + 8, CH), f32), v((2, CH, HALF), f32),
            *map(msg, (2 * WB, 4 * W2, 2 * W1, 2 * W1, 2 * W1, 2 * W2, 2 * W2, W1, W1, W2, W2, W1 + W2, W1 + W2)),
            pltpu.SemaphoreType.DMA((len(KINDS), KEEP)), pltpu.SemaphoreType.DMA((len(KINDS), KEEP)), pltpu.SemaphoreType.DMA((NS,)),
            pltpu.SemaphoreType.DMA((KEEP,)), pltpu.SemaphoreType.DMA((KEEP,)), pltpu.SemaphoreType.DMA,
            pltpu.SemaphoreType.REGULAR((4,)),
        ],
        compiler_params=pltpu.CompilerParams(collective_id=cid, has_side_effects=True, vmem_limit_bytes=67043328),
        cost_estimate=pl.CostEstimate(flops=2 * ROWS * D * 4096, transcendentals=8 * ROWS * ROWS, bytes_accessed=2**30),
    )(x, gain, freq, wq, wk, wv, wo)


def solution(mesh, compute=True, comm=True):
    def step(x, gain, wq, wk, wv, wo):
        half = HEAD // 2
        freq = THETA ** (-jnp.arange(half, dtype=jnp.float32) / half)
        y, _ = call(x, gain[None], jnp.concatenate([freq, freq])[None], wq, wk, wv, wo, compute=compute, comm=comm)
        return y

    tokens, columns = P("dp", None), P(None, "tp")
    return jax.shard_map(step, mesh=mesh, in_specs=(tokens, P(None), columns, columns, columns, P("tp", None)), out_specs=tokens, check_vma=False)
```

```python
import functools

import jax
import jax.numpy as jnp
from jax import lax
from jax.experimental import pallas as pl
from jax.experimental.pallas import tpu as pltpu
from jax.sharding import PartitionSpec as P

HEAD = 128
THETA = 10000
NEG = -1e30
LOG2E = 1.4426950408889634
MESH = pl.DeviceIdType.MESH

ROWS = 2048
D = 16384
MINE = 1024
PAIR = 2 * MINE
HALF = 8192
SIZES = ((1152, 896, 256), (1280, 768, 512))
BOTH = 2048
M1, M2, MB = map(max, zip(*SIZES))
EARLY = 2
CH = 256
SUB = 16
PER = CH // SUB
NCH = ROWS // CH
NSUB = ROWS // SUB
KEEP = 4
KS, TN = 4096, 512
NS = 3
FIRST = BOTH // TN
TALL, WIDE = 16, 2048
QT, QK = 3 * 1024 // TN, D // KS
UQ = QT * QK
UO = HALF // (2 * TN)
UNITS = UQ + UO
KINDS = (BB, Y1, E2, E1, X2, X1, Y2, FP, FX, FY, AP, AY, CP, CX, EY0, EY1, SIB, SEEN, NORM, WO) = range(20)
LAG = 2
STAGES = 8
ATT, OUT = 10, 12


def _dot(a, b, ca, cb):
    return lax.dot_general(a, b, (((ca,), (cb,)), ((), ())), preferred_element_type=jnp.float32)


def kernel(x, gain, freq, wq, wk, wv, wo, y, wos,
           a, w, acc, csv, gain8, q_s, k_s, v_s, seen, top_s, mix_s, term,
           bb, be2, be1, sy1, ry1, sx2, rx2, sx1, rx1, sy2, ry2, fin, res,
           ssem, rsem, wsem, lsem, rssem, xsem, credit, *, compute, comm):
    t = lax.axis_index("tp")
    yy, z, core = t // 8, lax.rem(t // 2, 4), lax.rem(t, 2)
    mid = (z == 1) | (z == 2)
    end = jnp.logical_not(mid)
    s = z // 2
    yo, so = 1 - yy, 1 - s
    to_y = yo * 8 + z * 2 + core
    to_p = yy * 8 + (z + 1 - 2 * lax.rem(z, 2)) * 2 + core
    to_x = yy * 8 + jnp.where(mid, 3 - z, z) * 2 + core
    to_s = yy * 8 + z * 2 + 1 - core

    def greet(act):
        for n, dev in enumerate((to_y, to_p, to_s)):
            act(n, dev)

        @pl.when(mid)
        def _():
            act(3, to_x)

    def signal(sem, dev):
        pl.semaphore_signal(sem, inc=1, device_id={"tp": dev}, device_id_type=MESH)

    bar = pltpu.get_barrier_semaphore()
    greet(lambda n, dev: signal(bar, dev))

    def rc(kind, slot, src, dst, dev):
        return pltpu.make_async_remote_copy(src_ref=src, dst_ref=dst, send_sem=ssem.at[kind, slot], recv_sem=rsem.at[kind, slot],
                                            device_id={"tp": dev}, device_id_type=MESH)

    def cols(at, n):
        return pl.ds(pl.multiple_of(at, 128), n)

    mine, other = core * HALF, (1 - core) * HALF

    def t1(r, p):
        return (2 * r + p) * BOTH

    def exchange(m, full, sizes):
        parts = {None: [], "mid": [], "end": []}
        w1, w2, wb = sizes
        wa = w1 - wb

        def t2(r, p):
            return t1(r, p) + w1

        def stage(n, who=None):
            return lambda body: parts[who].append((LAG * n, body))

        def emit():
            for who, bodies in parts.items():
                def run(bodies=bodies):
                    for o, body in bodies:
                        go = functools.partial(body, Stage(m - o))
                        if full:
                            go()
                        else:
                            pl.when((m >= o) & (m < NSUB + o))(go)

                if who is None:
                    run()
                else:
                    pl.when(mid if who == "mid" else end)(run)
                bodies.clear()

        class Stage:
            def __init__(self, j):
                self.j, self.slot = j, lax.rem(j, KEEP)
                self.rows = pl.ds(pl.multiple_of(j * SUB, SUB), SUB)

            def y(self, at, n, first=mine):
                return y.at[self.rows, cols(first + at, n)]

            def term(self, at, n):
                rows = pl.ds(pl.multiple_of(lax.rem(self.j, PER) * SUB, SUB), SUB)
                return term.at[lax.rem(self.j // PER, 2), rows, cols(at, n)]

            def buf(self, ref, at, n):
                return ref.at[self.slot, :, cols(at, n)]

            def wide(self, ref, at, n):
                return self.buf(ref, at, n)[...].astype(jnp.float32)

            def copy(self, kind, src, dst=None, dev=to_y):
                return rc(kind, self.slot, src, src if dst is None else dst, dev)

            def send(self, kind, dev, src, dst=None):
                self.copy(kind, src, dst, dev).start()

            def got(self, kind, ref):
                self.copy(kind, ref).wait_recv()

            def gone(self, kind, ref):
                self.copy(kind, ref).wait_send()

            def residual(self):
                return pltpu.make_async_copy(x.at[self.rows, cols(mine + t1(yy, s), BOTH)], self.buf(res, 0, BOTH), rssem.at[self.slot])

            def keep(self):
                return pltpu.make_async_copy(self.buf(fin, 0, BOTH), self.y(t1(yy, s), BOTH), lsem.at[self.slot])

        low = jnp.bfloat16

        def grow(e, at, n, more):
            own = e.term(at, n)
            own[...] = own[...] + more

        @stage(0, "mid")
        def _(e):
            for p in range(2):
                e.buf(bb, p * wb, wb)[...] = e.term(t1(yo, p), wb)[...].astype(low)

        @stage(1, "mid")
        def _(e):
            e.gone(BB, e.buf(bb, 0, 2 * wb))
            for p in range(2):
                e.buf(sy1, p * wa, wa)[...] = e.term(t1(yo, p) + wb, wa)[...].astype(low)

        @stage(1, "end")
        def _(e):
            e.got(BB, e.buf(bb, 0, 2 * wb))
            for p in range(2):
                e.buf(sy1, p * w1, wb)[...] = (e.term(t1(yo, p), wb)[...] + e.wide(bb, p * wb, wb)).astype(low)
                e.buf(sy1, p * w1 + wb, wa)[...] = e.term(t1(yo, p) + wb, wa)[...].astype(low)
            for q in range(4):
                e.buf(be2, q * w2, w2)[...] = e.term(t2(0, q), w2)[...].astype(low)

        @stage(2, "mid")
        def _(e):
            e.gone(Y1, e.buf(sy1, 0, 2 * wa))
            e.got(Y1, e.buf(ry1, 0, 2 * wa))
            e.got(E2, e.buf(be2, 0, 4 * w2))
            for p in range(2):
                grow(e, t1(yy, p) + wb, wa, e.wide(ry1, p * wa, wa))
            for r in range(2):
                e.buf(sx2, r * w2, w2)[...] = (e.term(t2(r, so), w2)[...] + e.wide(be2, (2 * r + so) * w2, w2)).astype(low)
                grow(e, t2(r, s), w2, e.wide(be2, (2 * r + s) * w2, w2))

        @stage(2, "end")
        def _(e):
            e.gone(Y1, e.buf(sy1, 0, 2 * w1))
            e.got(Y1, e.buf(ry1, 0, 2 * w1))
            e.gone(E2, e.buf(be2, 0, 4 * w2))
            for p in range(2):
                e.buf(be1, p * w1, w1)[...] = (e.term(t1(yy, p), w1)[...] + e.wide(ry1, p * w1, w1)).astype(low)

        @stage(3, "end")
        def _(e):
            e.gone(E1, e.buf(be1, 0, 2 * w1))

        @stage(3, "mid")
        def _(e):
            e.gone(X2, e.buf(sx2, 0, 2 * w2))
            e.got(E1, e.buf(be1, 0, 2 * w1))
            e.buf(sx1, 0, w1)[...] = (e.term(t1(yy, so), w1)[...] + e.wide(be1, so * w1, w1)).astype(low)
            grow(e, t1(yy, s), w1, e.wide(be1, s * w1, w1))
            e.got(X2, e.buf(rx2, 0, 2 * w2))
            e.buf(sy2, 0, w2)[...] = (e.term(t2(yo, s), w2)[...] + e.wide(rx2, yo * w2, w2)).astype(low)
            grow(e, t2(yy, s), w2, e.wide(rx2, yy * w2, w2))

        @stage(4, "mid")
        def _(e):
            e.gone(X1, e.buf(sx1, 0, w1))
            e.gone(Y2, e.buf(sy2, 0, w2))
            e.residual().wait()
            e.got(X1, e.buf(rx1, 0, w1))
            e.got(Y2, e.buf(ry2, 0, w2))
            for at, n, ref in ((0, w1, rx1), (w1, w2, ry2)):
                e.buf(fin, at, n)[...] = (e.term(t1(yy, s) + at, n)[...] + e.wide(ref, 0, n) + e.wide(res, at, n)).astype(low)

        @stage(5, "mid")
        def _(e):
            for kind in (FP, FX, FY):
                e.gone(kind, e.buf(fin, 0, BOTH))
            e.keep().wait()
            e.got(FX, e.y(t1(yy, so), BOTH))
            e.got(FY, e.y(t1(yo, s), BOTH))

        @stage(5, "end")
        def _(e):
            e.got(FP, e.y(t1(yy, s), BOTH))

        @stage(6, "mid")
        def _(e):
            e.gone(AP, e.y(0, BOTH))
            e.gone(AY, e.y(0, w1))
            e.gone(CP, e.y(0, w2))
            e.gone(CX, e.y(0, w2))
            e.got(AY, e.y(t1(yo, so), w1))
            e.got(CX, e.y(t2(yo, so), w2))

        @stage(6, "end")
        def _(e):
            e.gone(EY0, e.y(0, w1))
            e.got(AP, e.y(t1(yy, so), BOTH))
            e.got(CP, e.y(t2(yo, s), w2))
            e.got(EY0, e.y(t1(yo, s), w1))

        @stage(7, "end")
        def _(e):
            e.gone(EY1, e.y(0, BOTH))
            e.got(EY1, e.y(t1(yo, so), BOTH))

        @stage(8)
        def _(e):
            e.gone(SIB, e.y(0, HALF))
            e.got(SIB, e.y(0, HALF, other))

        emit()

        def spend():
            greet(lambda n, dev: pl.semaphore_wait(credit.at[n], 1))

        spend() if full else pl.when(m >= LAG)(spend)

        @stage(0, "mid")
        def _(e):
            e.send(BB, to_p, e.buf(bb, 0, 2 * wb))

        @stage(1, "end")
        def _(e):
            e.send(Y1, to_y, e.buf(sy1, 0, 2 * w1), e.buf(ry1, 0, 2 * w1))
            e.send(E2, to_p, e.buf(be2, 0, 4 * w2))

        @stage(1, "mid")
        def _(e):
            e.send(Y1, to_y, e.buf(sy1, 0, 2 * wa), e.buf(ry1, 0, 2 * wa))

        @stage(2, "end")
        def _(e):
            e.send(E1, to_p, e.buf(be1, 0, 2 * w1))

        @stage(2, "mid")
        def _(e):
            e.send(X2, to_x, e.buf(sx2, 0, 2 * w2), e.buf(rx2, 0, 2 * w2))

        @stage(3, "mid")
        def _(e):
            e.send(X1, to_x, e.buf(sx1, 0, w1), e.buf(rx1, 0, w1))
            e.send(Y2, to_y, e.buf(sy2, 0, w2), e.buf(ry2, 0, w2))
            e.residual().start()

        @stage(4, "mid")
        def _(e):
            for kind, dev in ((FP, to_p), (FX, to_x), (FY, to_y)):
                e.send(kind, dev, e.buf(fin, 0, BOTH), e.y(t1(yy, s), BOTH))
            e.keep().start()

        @stage(5, "mid")
        def _(e):
            e.send(AP, to_p, e.y(t1(yy, so), BOTH))
            e.send(CX, to_x, e.y(t2(yo, s), w2))
            e.send(AY, to_y, e.y(t1(yy, so), w1))
            e.send(CP, to_p, e.y(t2(yo, s), w2))

        @stage(5, "end")
        def _(e):
            e.send(EY0, to_y, e.y(t1(yy, s), w1))

        @stage(6, "end")
        def _(e):
            e.send(EY1, to_y, e.y(t1(yy, so), BOTH))

        @stage(7)
        def _(e):
            e.send(SIB, to_s, e.y(0, HALF))

        emit()
        greet(lambda n, dev: signal(credit.at[n], dev))

    wo_sent = rc(WO, 0, wo.at[:, cols(other, HALF)], wos, to_s)

    def out_cols(n):
        n = jnp.where(n == 1, FIRST, jnp.where((n > 1) & (n <= FIRST), n - 1, n))
        return lax.rem(n + 2 * FIRST * yo, HALF // TN) * TN

    def tiles(g):
        u, k = lax.rem(g, UNITS), lax.rem(g, NS)

        def proj(ref, n):
            @pl.when((u >= n * (UQ // 3)) & (u < (n + 1) * (UQ // 3)))
            def _():
                v = u - n * (UQ // 3)
                pltpu.make_async_copy(ref.at[pl.ds(pl.multiple_of(lax.rem(v, QK) * KS, KS), KS), cols(v // QK * TN, TN)], w.at[k], wsem.at[k]).start()

        @pl.when(g < NCH * UNITS)
        def _():
            for n, ref in enumerate((wq, wk, wv)):
                proj(ref, n)

            @pl.when(u >= UQ)
            def _():
                @pl.when(g == UQ)
                def _():
                    wo_sent.wait_recv()

                for n in range(2):
                    v = out_cols(2 * (u - UQ) + n)
                    for ref, at, row in ((wo, mine, 0), (wos, 0, MINE)):
                        src = ref.at[:, cols(at + v, TN)]
                        pltpu.make_async_copy(src, w.at[k, pl.ds(n * PAIR + row, MINE)], wsem.at[k]).start()

    def tile(g):
        k = lax.rem(g, NS)
        pltpu.make_async_copy(w.at[k], w.at[k], wsem.at[k]).wait()
        return w.at[k]

    def rows_of(c):
        return pl.ds(pl.multiple_of(c * CH, CH), CH)

    own_rows, other_rows = (pl.ds(pl.multiple_of(k * (CH // 2), CH // 2), CH // 2) for k in (core, 1 - core))

    def fetch(c):
        rows = pl.ds(pl.multiple_of(c * CH + core * (CH // 2), CH // 2), CH // 2)
        return pltpu.make_async_copy(x.at[rows], a.at[own_rows], xsem.at[0])

    def first_rows(n):
        rows = pl.ds(n * (CH // 4), CH // 4)
        return pltpu.make_async_copy(x.at[rows], a.at[rows], xsem.at[n])

    def angles(c):
        place = c * CH + lax.broadcasted_iota(jnp.int32, (CH, HEAD), 0)
        angle = place.astype(jnp.float32) * freq[...]
        first = lax.broadcasted_iota(jnp.int32, (CH, HEAD), 1) < HEAD // 2
        sin = jnp.sin(angle)
        csv[:, :HEAD] = jnp.cos(angle)
        csv[:, HEAD:] = jnp.where(first, -sin, sin)

    def norm(first, last):
        def group(r, _):
            rows = pl.ds(pl.multiple_of(r * TALL, TALL), TALL)
            total = jnp.zeros((TALL, HEAD), jnp.float32)
            for n in range(D // WIDE):
                wide = a[rows, n * WIDE:(n + 1) * WIDE].astype(jnp.float32)
                sq = wide * wide
                for i in range(WIDE // HEAD):
                    total = total + sq[:, i * HEAD:(i + 1) * HEAD]
            scale = lax.rsqrt(jnp.sum(total, -1, keepdims=True) * (1 / D) + 1e-6)
            for n in range(D // WIDE):
                at = slice(n * WIDE, (n + 1) * WIDE)
                a[rows, at] = (a[rows, at].astype(jnp.float32) * scale * jnp.concatenate([gain8[:, at]] * (TALL // 8))).astype(jnp.bfloat16)
            return None

        lax.fori_loop(first // TALL, last // TALL, group, None)

    def turn(b):
        b = b.astype(jnp.float32)
        return (b * csv[:, :HEAD] + pltpu.roll(b, HEAD // 2, 1) * csv[:, HEAD:]).astype(jnp.bfloat16)

    def project(c, u, _):
        g = c * UNITS + u
        ref = tile(g)
        ks, n = lax.rem(u, QK), u // QK
        acc[...] += jnp.dot(a[:, cols(ks * KS, KS)], ref[...], preferred_element_type=jnp.float32)
        tiles(g + NS)

        @pl.when(ks == QK - 1)
        def _():
            heads = [(lax.rem(n, 2) * (TN // HEAD) + i, slice(i * HEAD, (i + 1) * HEAD)) for i in range(TN // HEAD)]

            @pl.when(n < 2)
            def _():
                for h, at in heads:
                    q_s[h] = turn(acc[:, at].astype(jnp.bfloat16))

            @pl.when((n >= 2) & (n < 4))
            def _():
                for h, at in heads:
                    k_s[h, rows_of(c), :] = turn(acc[:, at].astype(jnp.bfloat16))

            @pl.when(n >= 4)
            def _():
                for h, at in heads:
                    v_s[h, :, cols(c * CH, CH)] = acc[:, at].astype(jnp.bfloat16).T

            acc[...] = jnp.zeros_like(acc)
        return None

    def attend(c, h0, count):
        e = HEAD**-0.5 * LOG2E
        for i in range(count):
            top_s[i:i + 1, :] = jnp.full((1, CH), NEG, jnp.float32)
            mix_s[i] = jnp.zeros((HEAD + 8, CH), jnp.float32)
        ones = jnp.ones((8, CH), jnp.bfloat16)

        def block(j, masked):
            here = pl.ds(pl.multiple_of(j * CH, CH), CH)
            scores = [_dot(k_s[h0 + i, here, :], q_s[h0 + i], 1, 1) for i in range(count)]
            if masked:
                ok = lax.broadcasted_iota(jnp.int32, (CH, CH), 1) >= lax.broadcasted_iota(jnp.int32, (CH, CH), 0)
            weights, keeps = [], []
            for i, sc in enumerate(scores):
                if masked:
                    sc = jnp.where(ok, sc, 2 * NEG)
                old = top_s[i:i + 1, :]
                top = jnp.maximum(old, sc.max(axis=0, keepdims=True))
                top_s[i:i + 1, :] = top
                weights.append(jnp.exp2((sc - top) * e).astype(jnp.bfloat16))
                keeps.append(jnp.exp2((old - top) * e))
            for i, (p, kp) in enumerate(zip(weights, keeps)):
                values = jnp.concatenate([v_s[h0 + i, :, here], ones], axis=0)
                mix_s[i] = mix_s[i] * kp + _dot(values, p, 1, 0)

        lax.fori_loop(0, c, lambda j, _: block(j, False), None)
        block(c, True)
        for i in range(count):
            out = mix_s[i, :HEAD, :] * (1 / mix_s[i, HEAD:HEAD + 1, :])
            seen[:, cols((h0 + i) * HEAD, HEAD)] = out.T.astype(jnp.bfloat16)

    def out_tile(c, v, _):
        g = c * UNITS + UQ + v
        ref = tile(g)
        for n in range(2):
            part = jnp.dot(seen[...], ref[n * PAIR:(n + 1) * PAIR], preferred_element_type=jnp.float32)
            term[lax.rem(c, 2), :, cols(out_cols(2 * v + n), TN)] = part
        tiles(g + NS)
        return None

    norm_sent = rc(NORM, 0, a.at[own_rows], a.at[own_rows], to_s)
    norm_got = rc(NORM, 0, a.at[other_rows], a.at[other_rows], to_s)
    seen_sent = rc(SEEN, 0, seen.at[:, pl.ds(0, 1024)], seen.at[:, pl.ds(1024, 1024)], to_s)

    if compute:
        for n in range(4):
            first_rows(n).start()
        for g in range(NS):
            tiles(g)
        acc[...] = jnp.zeros_like(acc)
        gain8[...] = jnp.broadcast_to(gain[...].astype(jnp.float32), gain8.shape)

    @pl.when(mid)
    def _():
        pl.semaphore_wait(bar, 4)

    @pl.when(end)
    def _():
        pl.semaphore_wait(bar, 3)

    if compute:
        wo_sent.start()

    def step(n, _):
        c, i = n // PER, lax.rem(n, PER)
        if compute:
            @pl.when((c < NCH) & (i == OUT))
            def _():
                seen_sent.start()

        if comm:
            m = (c - 1) * PER + i + EARLY
            full = (m >= LAG * STAGES) & (m < NSUB)
            for odd, sizes in enumerate(SIZES):
                turn_ = (m >= 0) & (lax.rem(m + LAG, 2) == odd)
                pl.when(turn_ & full)(functools.partial(exchange, m, True, sizes))
                pl.when(turn_ & jnp.logical_not(full))(functools.partial(exchange, m, False, sizes))

        def slot(first, last):
            return pl.when((c < NCH) & (i >= first) & (i < last))

        if compute:
            @slot(0, 1)
            def _():
                angles(c)

                @pl.when(c == 0)
                def _():
                    def piece(n, _):
                        first_rows(n).wait()
                        norm(n * (CH // 4), (n + 1) * (CH // 4))
                        return None

                    lax.fori_loop(0, 4, piece, None)

                @pl.when(c > 0)
                def _():
                    norm_got.wait_recv()
                    norm_sent.wait_send()

            @slot(0, ATT)
            def _():
                lax.fori_loop(i * UQ // ATT, (i + 1) * UQ // ATT, functools.partial(project, c), None)

            @slot(ATT, ATT + 1)
            def _():
                @pl.when(c < NCH - 1)
                def _():
                    fetch(c + 1).start()

            @slot(ATT, OUT)
            def _():
                attend(c, (i - ATT) * (8 // (OUT - ATT)), 8 // (OUT - ATT))

            @slot(OUT, OUT + 1)
            def _():
                @pl.when(c < NCH - 1)
                def _():
                    fetch(c + 1).wait()
                    norm(core * (CH // 2), (core + 1) * (CH // 2))

                seen_sent.wait_recv()
                seen_sent.wait_send()

                @pl.when(c < NCH - 1)
                def _():
                    norm_sent.start()

                out_tile(c, 0, None)

            @slot(OUT + 1, PER)
            def _():
                k, n = i - OUT - 1, PER - OUT - 1
                lax.fori_loop(1 + k * (UO - 1) // n, 1 + (k + 1) * (UO - 1) // n, functools.partial(out_tile, c), None)

        return None

    steps = NSUB + LAG * (STAGES + 1) - EARLY
    lax.fori_loop(0, PER + (steps if comm else NSUB - PER), step, None)
    if comm:
        greet(lambda n, dev: pl.semaphore_wait(credit.at[n], LAG))
    if compute:
        wo_sent.wait_send()


def call(x, gain, freq, wq, wk, wv, wo, compute=True, comm=True, cid=0):
    any_, vmem = pl.BlockSpec(memory_space=pl.ANY), pl.BlockSpec(memory_space=pltpu.VMEM)
    low = jnp.bfloat16
    v, f32 = pltpu.VMEM, jnp.float32
    msg = lambda n: v((KEEP, SUB, n), low)
    return pl.pallas_call(
        functools.partial(kernel, compute=compute, comm=comm),
        out_shape=[jax.ShapeDtypeStruct((ROWS, D), low), jax.ShapeDtypeStruct((1024, HALF), low)],
        in_specs=[any_, vmem, vmem] + [any_] * 4,
        out_specs=[any_, any_],
        scratch_shapes=[
            v((CH, D), low), v((NS, KS, TN), low), v((CH, TN), f32), v((CH, 2 * HEAD), f32), v((8, D), f32),
            v((8, CH, HEAD), low), v((8, ROWS, HEAD), low), v((8, HEAD, ROWS), low), v((CH, 2048), low),
            v((8, CH), f32), v((4, HEAD + 8, CH), f32), v((2, CH, HALF), f32),
            *map(msg, (2 * MB, 4 * M2, 2 * M1, 2 * M1, 2 * M1, 2 * M2, 2 * M2, M1, M1, M2, M2, BOTH, BOTH)),
            pltpu.SemaphoreType.DMA((len(KINDS), KEEP)), pltpu.SemaphoreType.DMA((len(KINDS), KEEP)), pltpu.SemaphoreType.DMA((NS,)),
            pltpu.SemaphoreType.DMA((KEEP,)), pltpu.SemaphoreType.DMA((KEEP,)), pltpu.SemaphoreType.DMA((4,)),
            pltpu.SemaphoreType.REGULAR((4,)),
        ],
        compiler_params=pltpu.CompilerParams(collective_id=cid, has_side_effects=True, vmem_limit_bytes=67043328),
        cost_estimate=pl.CostEstimate(flops=2 * ROWS * D * 4096, transcendentals=8 * ROWS * ROWS, bytes_accessed=2**30),
    )(x, gain, freq, wq, wk, wv, wo)


def solution(mesh, compute=True, comm=True):
    def step(x, gain, wq, wk, wv, wo):
        half = HEAD // 2
        freq = THETA ** (-jnp.arange(half, dtype=jnp.float32) / half)
        y, _ = call(x, gain[None], jnp.concatenate([freq, freq])[None], wq, wk, wv, wo, compute=compute, comm=comm)
        return y

    tokens, columns = P("dp", None), P(None, "tp")
    return jax.shard_map(step, mesh=mesh, in_specs=(tokens, P(None), columns, columns, columns, P("tp", None)), out_specs=tokens, check_vma=False)
```

```python
import functools

import jax
import jax.numpy as jnp
from jax import lax
from jax.experimental import pallas as pl
from jax.experimental.pallas import tpu as pltpu
from jax.sharding import PartitionSpec as P

HEAD = 128
THETA = 10000
NEG = float(jnp.finfo(jnp.float32).min)
LOG2E = 1.4426950408889634
MESH = pl.DeviceIdType.MESH

ROWS = 2048
D = 16384
MINE = 1024
HALF = 8192
SIZES = ((1152, 896, 256), (1280, 768, 512))
BOTH = 2048
M1, M2, MB = map(max, zip(*SIZES))
CH = 256
SUB = 16
PER = CH // SUB
NCH = ROWS // CH
NSUB = ROWS // SUB
KEEP = 8
KS, TN = 2048, 1024
NS = 4
FIRST = BOTH // TN
TALL, WIDE = 16, 2048
QT, QK = 3 * 1024 // TN, D // KS
UQ = QT * QK
UO = HALF // TN
PART = QT // 3
UNITS = UQ + UO
KINDS = (BB, Y1, E2, E1, X2, X1, Y2, FP, FX, FY, AP, AY, CP, CX, EY0, EY1, SIB, SEEN, NORM, WO) = range(20)
LAG = 2
STAGES = 8
FAST = 3
EARLY = 2
LATE = NSUB - CH // SUB + EARLY
ATT, OUT = 10, 12


def _dot(a, b, ca, cb):
    return lax.dot_general(a, b, (((ca,), (cb,)), ((), ())), preferred_element_type=jnp.float32)


def kernel(x, gain, freq, wq, wk, wv, wo, y, wos,
           a, w, acc, csv, gain8, q_s, k_s, v_s, seen, top_s, mix_s, term,
           bb, be2, be1, sy1, ry1, sx2, rx2, sx1, rx1, sy2, ry2, fin, res,
           ssem, rsem, wsem, lsem, rssem, xsem, credit, *, compute, comm):
    t = lax.axis_index("tp")
    yy, z, core = t // 8, lax.rem(t // 2, 4), lax.rem(t, 2)
    mid = (z == 1) | (z == 2)
    end = jnp.logical_not(mid)
    s = z // 2
    yo, so = 1 - yy, 1 - s
    to_y = yo * 8 + z * 2 + core
    to_p = yy * 8 + (z + 1 - 2 * lax.rem(z, 2)) * 2 + core
    to_x = yy * 8 + jnp.where(mid, 3 - z, z) * 2 + core
    to_s = yy * 8 + z * 2 + 1 - core

    def greet(act):
        for n, dev in enumerate((to_y, to_p, to_s)):
            act(n, dev)

        @pl.when(mid)
        def _():
            act(3, to_x)

    def signal(sem, dev):
        pl.semaphore_signal(sem, inc=1, device_id={"tp": dev}, device_id_type=MESH)

    bar = pltpu.get_barrier_semaphore()
    greet(lambda n, dev: signal(bar, dev))

    def rc(kind, slot, src, dst, dev):
        return pltpu.make_async_remote_copy(src_ref=src, dst_ref=dst, send_sem=ssem.at[kind, slot], recv_sem=rsem.at[kind, slot],
                                            device_id={"tp": dev}, device_id_type=MESH)

    def cols(at, n):
        return pl.ds(pl.multiple_of(at, 128), n)

    mine, other = core * HALF, (1 - core) * HALF

    def t1(r, p):
        return (2 * r + p) * BOTH

    def exchange(m, odd, full=False, half=None, opens=True, closes=True):
        parts = {None: [], "mid": [], "end": []}
        delay, first, last = (2 * LAG, 0, LATE) if half is None else (FAST, LATE, NSUB)

        def stage(n, who=None):
            return lambda body: parts[who].append((n, body)) if half in (None, n % 2) else None

        def emit():
            for who, bodies in parts.items():
                def run(bodies=bodies):
                    for n, body in bodies:
                        o = delay * n // 2
                        go = functools.partial(body, Stage(m - o, *SIZES[(odd + o) % 2]))
                        if full:
                            go()
                        else:
                            pl.when((m >= first + o) & (m < last + o))(go)

                if who is None:
                    run()
                else:
                    pl.when(mid if who == "mid" else end)(run)
                bodies.clear()

        class Stage:
            def __init__(self, j, w1, w2, wb):
                self.w1, self.w2, self.wb, self.wa = w1, w2, wb, w1 - wb
                self.j, self.slot = j, lax.rem(j, KEEP)
                self.rows = pl.ds(pl.multiple_of(j * SUB, SUB), SUB)

            def t2(self, r, p):
                return t1(r, p) + self.w1

            def y(self, at, n, half=mine):
                return y.at[self.rows, cols(half + at, n)]

            def term(self, at, n):
                rows = pl.ds(pl.multiple_of(lax.rem(self.j, PER) * SUB, SUB), SUB)
                return term.at[lax.rem(self.j // PER, 2), rows, cols(at, n)]

            def buf(self, ref, at, n):
                return ref.at[self.slot, :, cols(at, n)]

            def wide(self, ref, at, n):
                return self.buf(ref, at, n)[...].astype(jnp.float32)

            def copy(self, kind, src, dst=None, dev=to_y):
                return rc(kind, self.slot, src, src if dst is None else dst, dev)

            def send(self, kind, dev, src, dst=None):
                self.copy(kind, src, dst, dev).start()

            def got(self, kind, ref):
                self.copy(kind, ref).wait_recv()

            def gone(self, kind, ref):
                self.copy(kind, ref).wait_send()

            def residual(self):
                return pltpu.make_async_copy(x.at[self.rows, cols(mine + t1(yy, s), BOTH)], self.buf(res, 0, BOTH), rssem.at[self.slot])

            def keep(self):
                return pltpu.make_async_copy(self.buf(fin, 0, BOTH), self.y(t1(yy, s), BOTH), lsem.at[self.slot])

        low = jnp.bfloat16

        def grow(e, at, n, more):
            own = e.term(at, n)
            own[...] = own[...] + more

        @stage(0, "mid")
        def _(e):
            for p in range(2):
                e.buf(bb, p * e.wb, e.wb)[...] = e.term(t1(yo, p), e.wb)[...].astype(low)

        @stage(1, "mid")
        def _(e):
            e.gone(BB, e.buf(bb, 0, 2 * e.wb))
            for p in range(2):
                e.buf(sy1, p * e.wa, e.wa)[...] = e.term(t1(yo, p) + e.wb, e.wa)[...].astype(low)

        @stage(1, "end")
        def _(e):
            e.got(BB, e.buf(bb, 0, 2 * e.wb))
            for p in range(2):
                e.buf(sy1, p * e.w1, e.wb)[...] = (e.term(t1(yo, p), e.wb)[...] + e.wide(bb, p * e.wb, e.wb)).astype(low)
                e.buf(sy1, p * e.w1 + e.wb, e.wa)[...] = e.term(t1(yo, p) + e.wb, e.wa)[...].astype(low)
            for q in range(4):
                e.buf(be2, q * e.w2, e.w2)[...] = e.term(e.t2(0, q), e.w2)[...].astype(low)

        @stage(2, "mid")
        def _(e):
            e.gone(Y1, e.buf(sy1, 0, 2 * e.wa))
            e.got(Y1, e.buf(ry1, 0, 2 * e.wa))
            e.got(E2, e.buf(be2, 0, 4 * e.w2))
            for p in range(2):
                grow(e, t1(yy, p) + e.wb, e.wa, e.wide(ry1, p * e.wa, e.wa))
            for r in range(2):
                e.buf(sx2, r * e.w2, e.w2)[...] = (e.term(e.t2(r, so), e.w2)[...] + e.wide(be2, (2 * r + so) * e.w2, e.w2)).astype(low)
                grow(e, e.t2(r, s), e.w2, e.wide(be2, (2 * r + s) * e.w2, e.w2))

        @stage(2, "end")
        def _(e):
            e.gone(Y1, e.buf(sy1, 0, 2 * e.w1))
            e.got(Y1, e.buf(ry1, 0, 2 * e.w1))
            e.gone(E2, e.buf(be2, 0, 4 * e.w2))
            for p in range(2):
                e.buf(be1, p * e.w1, e.w1)[...] = (e.term(t1(yy, p), e.w1)[...] + e.wide(ry1, p * e.w1, e.w1)).astype(low)

        @stage(3, "end")
        def _(e):
            e.gone(E1, e.buf(be1, 0, 2 * e.w1))

        @stage(3, "mid")
        def _(e):
            e.gone(X2, e.buf(sx2, 0, 2 * e.w2))
            e.got(E1, e.buf(be1, 0, 2 * e.w1))
            e.buf(sx1, 0, e.w1)[...] = (e.term(t1(yy, so), e.w1)[...] + e.wide(be1, so * e.w1, e.w1)).astype(low)
            grow(e, t1(yy, s), e.w1, e.wide(be1, s * e.w1, e.w1))
            e.got(X2, e.buf(rx2, 0, 2 * e.w2))
            e.buf(sy2, 0, e.w2)[...] = (e.term(e.t2(yo, s), e.w2)[...] + e.wide(rx2, yo * e.w2, e.w2)).astype(low)
            grow(e, e.t2(yy, s), e.w2, e.wide(rx2, yy * e.w2, e.w2))

        @stage(4, "mid")
        def _(e):
            e.gone(X1, e.buf(sx1, 0, e.w1))
            e.gone(Y2, e.buf(sy2, 0, e.w2))
            e.residual().wait()
            e.got(X1, e.buf(rx1, 0, e.w1))
            e.got(Y2, e.buf(ry2, 0, e.w2))
            for at, n, ref in ((0, e.w1, rx1), (e.w1, e.w2, ry2)):
                e.buf(fin, at, n)[...] = (e.term(t1(yy, s) + at, n)[...] + e.wide(ref, 0, n) + e.wide(res, at, n)).astype(low)

        @stage(5, "mid")
        def _(e):
            for kind in (FP, FX, FY):
                e.gone(kind, e.buf(fin, 0, BOTH))
            e.keep().wait()
            e.got(FX, e.y(t1(yy, so), BOTH))
            e.got(FY, e.y(t1(yo, s), BOTH))

        @stage(5, "end")
        def _(e):
            e.got(FP, e.y(t1(yy, s), BOTH))

        @stage(6, "mid")
        def _(e):
            e.gone(AP, e.y(0, BOTH))
            e.gone(AY, e.y(0, e.w1))
            e.gone(CP, e.y(0, e.w2))
            e.gone(CX, e.y(0, e.w2))
            e.got(AY, e.y(t1(yo, so), e.w1))
            e.got(CX, e.y(e.t2(yo, so), e.w2))

        @stage(6, "end")
        def _(e):
            e.gone(EY0, e.y(0, e.w1))
            e.got(AP, e.y(t1(yy, so), BOTH))
            e.got(CP, e.y(e.t2(yo, s), e.w2))
            e.got(EY0, e.y(t1(yo, s), e.w1))

        @stage(7, "end")
        def _(e):
            e.gone(EY1, e.y(0, BOTH))
            e.got(EY1, e.y(t1(yo, so), BOTH))

        @stage(8)
        def _(e):
            e.gone(SIB, e.y(0, HALF))
            e.got(SIB, e.y(0, HALF, other))

        emit()

        def spend():
            greet(lambda n, dev: pl.semaphore_wait(credit.at[n], 1))

        if opens:
            spend() if full else pl.when(m >= LAG)(spend)

        @stage(0, "mid")
        def _(e):
            e.send(BB, to_p, e.buf(bb, 0, 2 * e.wb))

        @stage(1, "end")
        def _(e):
            e.send(Y1, to_y, e.buf(sy1, 0, 2 * e.w1), e.buf(ry1, 0, 2 * e.w1))
            e.send(E2, to_p, e.buf(be2, 0, 4 * e.w2))

        @stage(1, "mid")
        def _(e):
            e.send(Y1, to_y, e.buf(sy1, 0, 2 * e.wa), e.buf(ry1, 0, 2 * e.wa))

        @stage(2, "end")
        def _(e):
            e.send(E1, to_p, e.buf(be1, 0, 2 * e.w1))

        @stage(2, "mid")
        def _(e):
            e.send(X2, to_x, e.buf(sx2, 0, 2 * e.w2), e.buf(rx2, 0, 2 * e.w2))

        @stage(3, "mid")
        def _(e):
            e.send(X1, to_x, e.buf(sx1, 0, e.w1), e.buf(rx1, 0, e.w1))
            e.send(Y2, to_y, e.buf(sy2, 0, e.w2), e.buf(ry2, 0, e.w2))
            e.residual().start()

        @stage(4, "mid")
        def _(e):
            for kind, dev in ((FP, to_p), (FX, to_x), (FY, to_y)):
                e.send(kind, dev, e.buf(fin, 0, BOTH), e.y(t1(yy, s), BOTH))
            e.keep().start()

        @stage(5, "mid")
        def _(e):
            e.send(AP, to_p, e.y(t1(yy, so), BOTH))
            e.send(CX, to_x, e.y(e.t2(yo, s), e.w2))
            e.send(AY, to_y, e.y(t1(yy, so), e.w1))
            e.send(CP, to_p, e.y(e.t2(yo, s), e.w2))

        @stage(5, "end")
        def _(e):
            e.send(EY0, to_y, e.y(t1(yy, s), e.w1))

        @stage(6, "end")
        def _(e):
            e.send(EY1, to_y, e.y(t1(yy, so), BOTH))

        @stage(7)
        def _(e):
            e.send(SIB, to_s, e.y(0, HALF))

        emit()
        if closes:
            greet(lambda n, dev: signal(credit.at[n], dev))

    wo_sent = rc(WO, 0, wo.at[:, cols(other, HALF)], wos, to_s)

    def out_cols(n):
        n = jnp.where(n == 1, FIRST, jnp.where((n > 1) & (n <= FIRST), n - 1, n))
        return lax.rem(n + 2 * FIRST * yo, HALF // TN) * TN

    def tiles(g):
        u, k = lax.rem(g, UNITS), lax.rem(g, NS)

        def proj(ref, n):
            @pl.when((u >= n * (UQ // 3)) & (u < (n + 1) * (UQ // 3)))
            def _():
                v = u - n * (UQ // 3)
                pltpu.make_async_copy(ref.at[pl.ds(pl.multiple_of(lax.rem(v, QK) * KS, KS), KS), cols(v // QK * TN, TN)], w.at[k], wsem.at[k]).start()

        @pl.when(g < NCH * UNITS)
        def _():
            for n, ref in enumerate((wq, wk, wv)):
                proj(ref, n)

            @pl.when(u >= UQ)
            def _():
                @pl.when(g == UQ)
                def _():
                    wo_sent.wait_recv()

                for ref, at, row in ((wo, mine, 0), (wos, 0, MINE)):
                    src = ref.at[:, cols(at + out_cols(u - UQ), TN)]
                    pltpu.make_async_copy(src, w.at[k, pl.ds(row, MINE)], wsem.at[k]).start()

    def tile(g):
        k = lax.rem(g, NS)
        pltpu.make_async_copy(w.at[k], w.at[k], wsem.at[k]).wait()
        return w.at[k]

    def rows_of(c):
        return pl.ds(pl.multiple_of(c * CH, CH), CH)

    own_rows, other_rows = (pl.ds(pl.multiple_of(k * (CH // 2), CH // 2), CH // 2) for k in (core, 1 - core))

    def fetch(c):
        rows = pl.ds(pl.multiple_of(c * CH + core * (CH // 2), CH // 2), CH // 2)
        return pltpu.make_async_copy(x.at[rows], a.at[own_rows], xsem.at[0])

    def first_rows(n):
        rows = pl.ds(n * (CH // 4), CH // 4)
        return pltpu.make_async_copy(x.at[rows], a.at[rows], xsem.at[n])

    def angles(c):
        place = c * CH + lax.broadcasted_iota(jnp.int32, (CH, HEAD), 0)
        angle = place.astype(jnp.float32) * freq[...]
        first = lax.broadcasted_iota(jnp.int32, (CH, HEAD), 1) < HEAD // 2
        sin = jnp.sin(angle)
        csv[:, :HEAD] = jnp.cos(angle)
        csv[:, HEAD:] = jnp.where(first, -sin, sin)

    def norm(first, last):
        def group(r, _):
            rows = pl.ds(pl.multiple_of(r * TALL, TALL), TALL)
            total = jnp.zeros((TALL, HEAD), jnp.float32)
            for n in range(D // WIDE):
                wide = a[rows, n * WIDE:(n + 1) * WIDE].astype(jnp.float32)
                sq = wide * wide
                for i in range(WIDE // HEAD):
                    total = total + sq[:, i * HEAD:(i + 1) * HEAD]
            scale = lax.rsqrt(jnp.sum(total, -1, keepdims=True) * (1 / D) + 1e-6)
            for n in range(D // WIDE):
                at = slice(n * WIDE, (n + 1) * WIDE)
                a[rows, at] = (a[rows, at].astype(jnp.float32) * scale * jnp.concatenate([gain8[:, at]] * (TALL // 8))).astype(jnp.bfloat16)
            return None

        lax.fori_loop(first // TALL, last // TALL, group, None)

    def turn(b):
        b = b.astype(jnp.float32)
        return (b * csv[:, :HEAD] + pltpu.roll(b, HEAD // 2, 1) * csv[:, HEAD:]).astype(jnp.bfloat16)

    def project(c, u, _):
        g = c * UNITS + u
        ref = tile(g)
        ks, n = lax.rem(u, QK), u // QK
        acc[...] += jnp.dot(a[:, cols(ks * KS, KS)], ref[...], preferred_element_type=jnp.float32)
        tiles(g + NS)

        @pl.when(ks == QK - 1)
        def _():
            heads = [(lax.rem(n, PART) * (TN // HEAD) + i, slice(i * HEAD, (i + 1) * HEAD)) for i in range(TN // HEAD)]

            @pl.when(n < PART)
            def _():
                for h, at in heads:
                    q_s[h] = turn(acc[:, at].astype(jnp.bfloat16))

            @pl.when((n >= PART) & (n < 2 * PART))
            def _():
                for h, at in heads:
                    k_s[h, rows_of(c), :] = turn(acc[:, at].astype(jnp.bfloat16))

            @pl.when(n >= 2 * PART)
            def _():
                for h, at in heads:
                    v_s[h, :, cols(c * CH, CH)] = acc[:, at].astype(jnp.bfloat16).T

            acc[...] = jnp.zeros_like(acc)
        return None

    def attend(c, h0, count):
        e = HEAD**-0.5 * LOG2E
        for i in range(count):
            top_s[i:i + 1, :] = jnp.full((1, CH), NEG, jnp.float32)
            mix_s[i] = jnp.zeros((HEAD + 8, CH), jnp.float32)
        ones = jnp.ones((8, CH), jnp.bfloat16)

        def block(j, masked):
            here = pl.ds(pl.multiple_of(j * CH, CH), CH)
            scores = [_dot(k_s[h0 + i, here, :], q_s[h0 + i], 1, 1) for i in range(count)]
            if masked:
                ok = lax.broadcasted_iota(jnp.int32, (CH, CH), 1) >= lax.broadcasted_iota(jnp.int32, (CH, CH), 0)
            weights, keeps = [], []
            for i, sc in enumerate(scores):
                if masked:
                    sc = jnp.where(ok, sc, -jnp.inf)
                old = top_s[i:i + 1, :]
                top = jnp.maximum(old, sc.max(axis=0, keepdims=True))
                top_s[i:i + 1, :] = top
                weights.append(jnp.exp2((sc - top) * e).astype(jnp.bfloat16))
                keeps.append(jnp.exp2((old - top) * e))
            for i, (p, kp) in enumerate(zip(weights, keeps)):
                values = jnp.concatenate([v_s[h0 + i, :, here], ones], axis=0)
                mix_s[i] = mix_s[i] * kp + _dot(values, p, 1, 0)

        lax.fori_loop(0, c, lambda j, _: block(j, False), None)
        block(c, True)
        for i in range(count):
            out = mix_s[i, :HEAD, :] * (1 / mix_s[i, HEAD:HEAD + 1, :])
            seen[:, cols((h0 + i) * HEAD, HEAD)] = out.T.astype(jnp.bfloat16)

    def out_tile(c, v, _):
        g = c * UNITS + UQ + v
        ref = tile(g)
        term[lax.rem(c, 2), :, cols(out_cols(v), TN)] = jnp.dot(seen[...], ref[...], preferred_element_type=jnp.float32)
        tiles(g + NS)
        return None

    norm_sent = rc(NORM, 0, a.at[own_rows], a.at[own_rows], to_s)
    norm_got = rc(NORM, 0, a.at[other_rows], a.at[other_rows], to_s)
    seen_sent = rc(SEEN, 0, seen.at[:, pl.ds(0, 1024)], seen.at[:, pl.ds(1024, 1024)], to_s)

    if compute:
        for n in range(4):
            first_rows(n).start()
        acc[...] = jnp.zeros_like(acc)
        gain8[...] = jnp.broadcast_to(gain[...].astype(jnp.float32).reshape(1, D), gain8.shape)

        def piece(n, _):
            first_rows(n).wait()

            @pl.when(n == 1)
            def _():
                for g in range(NS):
                    tiles(g)

            norm(n * (CH // 4), (n + 1) * (CH // 4))
            return None

        lax.fori_loop(0, 4, piece, None)

    @pl.when(mid)
    def _():
        pl.semaphore_wait(bar, 4)

    @pl.when(end)
    def _():
        pl.semaphore_wait(bar, 3)

    if compute:
        wo_sent.start()

    def step(n, _):
        c, i = n // PER, lax.rem(n, PER)
        if compute:
            @pl.when((c < NCH) & (i == OUT))
            def _():
                seen_sent.start()

        if comm:
            m = (c - 1) * PER + i + EARLY
            full = m >= LAG * STAGES
            for odd in range(2):
                now = (m >= 0) & (lax.rem(m + LAG, 2) == odd)
                pl.when(now & full)(functools.partial(exchange, m, odd, True))
                pl.when(now & jnp.logical_not(full))(functools.partial(exchange, m, odd))

        def slot(first, last):
            return pl.when((c < NCH) & (i >= first) & (i < last))

        if compute:
            @slot(0, 1)
            def _():
                angles(c)

                @pl.when(c > 0)
                def _():
                    norm_got.wait_recv()
                    norm_sent.wait_send()

            @slot(0, ATT)
            def _():
                lax.fori_loop(i * UQ // ATT, (i + 1) * UQ // ATT, functools.partial(project, c), None)

            @slot(ATT, ATT + 1)
            def _():
                @pl.when(c < NCH - 1)
                def _():
                    fetch(c + 1).start()

            @slot(ATT, OUT)
            def _():
                attend(c, (i - ATT) * (8 // (OUT - ATT)), 8 // (OUT - ATT))

            @slot(OUT, OUT + 1)
            def _():
                @pl.when(c < NCH - 1)
                def _():
                    fetch(c + 1).wait()
                    norm(core * (CH // 2), (core + 1) * (CH // 2))

                seen_sent.wait_recv()
                seen_sent.wait_send()

                @pl.when(c < NCH - 1)
                def _():
                    norm_sent.start()

                out_tile(c, 0, None)

            @slot(OUT + 1, PER)
            def _():
                k, n = i - OUT - 1, PER - OUT - 1
                lax.fori_loop(1 + k * (UO - 1) // n, 1 + (k + 1) * (UO - 1) // n, functools.partial(out_tile, c), None)

        return None

    def final(n, _):
        for odd in range(2):
            m = LATE + 2 * n + odd
            exchange(m, odd, closes=False)
            exchange(m, odd, half=0, opens=False, closes=False)
            exchange(m, odd, half=1, opens=False)
        return None

    lax.fori_loop(0, NCH * PER, step, None)
    if comm:
        lax.fori_loop(0, (NSUB + FAST * STAGES // 2 - LATE) // 2, final, None)
    if comm:
        greet(lambda n, dev: pl.semaphore_wait(credit.at[n], LAG))
    if compute:
        wo_sent.wait_send()


def call(x, gain, freq, wq, wk, wv, wo, compute=True, comm=True, cid=0):
    any_, vmem = pl.BlockSpec(memory_space=pl.ANY), pl.BlockSpec(memory_space=pltpu.VMEM)
    low = jnp.bfloat16
    v, f32 = pltpu.VMEM, jnp.float32
    msg = lambda n: v((KEEP, SUB, n), low)
    return pl.pallas_call(
        functools.partial(kernel, compute=compute, comm=comm),
        out_shape=[jax.ShapeDtypeStruct((ROWS, D), low), jax.ShapeDtypeStruct((1024, HALF), low)],
        in_specs=[any_, vmem, vmem] + [any_] * 4,
        out_specs=[any_, any_],
        scratch_shapes=[
            v((CH, D), low), v((NS, KS, TN), low), v((CH, TN), f32), v((CH, 2 * HEAD), f32), v((8, D), f32),
            v((8, CH, HEAD), low), v((8, ROWS, HEAD), low), v((8, HEAD, ROWS), low), v((CH, 2048), low),
            v((8, CH), f32), v((4, HEAD + 8, CH), f32), v((2, CH, HALF), f32),
            *map(msg, (2 * MB, 4 * M2, 2 * M1, 2 * M1, 2 * M1, 2 * M2, 2 * M2, M1, M1, M2, M2, BOTH, BOTH)),
            pltpu.SemaphoreType.DMA((len(KINDS), KEEP)), pltpu.SemaphoreType.DMA((len(KINDS), KEEP)), pltpu.SemaphoreType.DMA((NS,)),
            pltpu.SemaphoreType.DMA((KEEP,)), pltpu.SemaphoreType.DMA((KEEP,)), pltpu.SemaphoreType.DMA((4,)),
            pltpu.SemaphoreType.REGULAR((4,)),
        ],
        compiler_params=pltpu.CompilerParams(collective_id=cid, has_side_effects=True, vmem_limit_bytes=67043328),
        cost_estimate=pl.CostEstimate(flops=2 * ROWS * D * 4096, transcendentals=8 * ROWS * ROWS, bytes_accessed=2**30),
    )(x, gain, freq, wq, wk, wv, wo)


def solution(mesh, compute=True, comm=True):
    def step(x, gain, wq, wk, wv, wo):
        half = HEAD // 2
        freq = THETA ** (-jnp.arange(half, dtype=jnp.float32) / half)
        y, _ = call(x, gain, jnp.concatenate([freq, freq])[None], wq, wk, wv, wo, compute=compute, comm=comm)
        return y

    tokens, columns = P("dp", None), P(None, "tp")
    return jax.shard_map(step, mesh=mesh, in_specs=(tokens, P(None), columns, columns, columns, P("tp", None)), out_specs=tokens, check_vma=False)
```

```python
import functools

import jax
import jax.numpy as jnp
from jax import lax
from jax.experimental import pallas as pl
from jax.experimental.pallas import tpu as pltpu
from jax.sharding import PartitionSpec as P

HEAD = 128
THETA = 10000
NEG = float(jnp.finfo(jnp.float32).min)
LOG2E = 1.4426950408889634
MESH = pl.DeviceIdType.MESH

ROWS = 2048
D = 16384
MINE = 1024
HALF = 8192
SIZES = ((1152, 896, 256), (1280, 768, 512))
BOTH = 2048
M1, M2, MB = map(max, zip(*SIZES))
CH = 256
SUB = 16
PER = CH // SUB
NCH = ROWS // CH
NSUB = ROWS // SUB
KEEP = 8
KS, TN = 2048, 1024
NS = 4
FIRST = BOTH // TN
TALL, WIDE = 16, 2048
QT, QK = 3 * 1024 // TN, D // KS
UQ = QT * QK
UO = HALF // TN
PART = QT // 3
UNITS = UQ + UO
KINDS = (BB, Y1, E2, E1, X2, X1, Y2, FP, FX, FY, AP, AY, CP, CX, EY0, EY1, SIB, SEEN, NORM, WO) = range(20)
LAG = 2
STAGES = 8
FAST = 3
EARLY = 2
LATE = NSUB - CH // SUB + EARLY
VERY_LATE = NSUB - 7
ATT, OUT = 10, 12


def _dot(a, b, ca, cb):
    return lax.dot_general(a, b, (((ca,), (cb,)), ((), ())), preferred_element_type=jnp.float32)


def kernel(x, gain, freq, wq, wk, wv, wo, y, wos,
           a, w, acc, csv, gain8, q_s, k_s, v_s, seen, top_s, mix_s, term,
           bb, be2, be1, sy1, ry1, sx2, rx2, sx1, rx1, sy2, ry2, fin, res,
           ssem, rsem, wsem, lsem, rssem, xsem, credit, *, compute, comm):
    t = lax.axis_index("tp")
    yy, z, core = t // 8, lax.rem(t // 2, 4), lax.rem(t, 2)
    mid = (z == 1) | (z == 2)
    end = jnp.logical_not(mid)
    s = z // 2
    yo, so = 1 - yy, 1 - s
    to_y = yo * 8 + z * 2 + core
    to_p = yy * 8 + (z + 1 - 2 * lax.rem(z, 2)) * 2 + core
    to_x = yy * 8 + jnp.where(mid, 3 - z, z) * 2 + core
    to_s = yy * 8 + z * 2 + 1 - core

    def greet(act):
        for n, dev in enumerate((to_y, to_p, to_s)):
            act(n, dev)

        @pl.when(mid)
        def _():
            act(3, to_x)

    def signal(sem, dev):
        pl.semaphore_signal(sem, inc=1, device_id={"tp": dev}, device_id_type=MESH)

    bar = pltpu.get_barrier_semaphore()
    greet(lambda n, dev: signal(bar, dev))

    def rc(kind, slot, src, dst, dev):
        return pltpu.make_async_remote_copy(src_ref=src, dst_ref=dst, send_sem=ssem.at[kind, slot], recv_sem=rsem.at[kind, slot],
                                            device_id={"tp": dev}, device_id_type=MESH)

    def cols(at, n):
        return pl.ds(pl.multiple_of(at, 128), n)

    mine, other = core * HALF, (1 - core) * HALF

    def t1(r, p):
        return (2 * r + p) * BOTH

    def exchange(m, odd, full=False, half=None, opens=True, closes=True):
        parts = {None: [], "mid": [], "end": []}
        delay, first, last = (2 * LAG, 0, LATE) if half is None else (FAST, LATE, NSUB)

        def stage(n, who=None):
            return lambda body: parts[who].append((n, body)) if half in (None, n % 2) else None

        def emit():
            for who, bodies in parts.items():
                def run(bodies=bodies):
                    for n, body in bodies:
                        o = delay * n // 2
                        go = functools.partial(body, Stage(m - o, *SIZES[(odd + o) % 2]))
                        if full:
                            go()
                        else:
                            pl.when((m >= first + o) & (m < last + o))(go)

                if who is None:
                    run()
                else:
                    pl.when(mid if who == "mid" else end)(run)
                bodies.clear()

        class Stage:
            def __init__(self, j, w1, w2, wb):
                self.w1, self.w2, self.wb, self.wa = w1, w2, wb, w1 - wb
                self.j, self.slot = j, lax.rem(j, KEEP)
                self.rows = pl.ds(pl.multiple_of(j * SUB, SUB), SUB)

            def t2(self, r, p):
                return t1(r, p) + self.w1

            def last_hop(self, by_z, by_y):
                if half is None:
                    by_z()
                else:
                    pl.when(self.j < VERY_LATE)(by_z)
                    pl.when(self.j >= VERY_LATE)(by_y)

            def y(self, at, n, half=mine):
                return y.at[self.rows, cols(half + at, n)]

            def term(self, at, n):
                rows = pl.ds(pl.multiple_of(lax.rem(self.j, PER) * SUB, SUB), SUB)
                return term.at[lax.rem(self.j // PER, 2), rows, cols(at, n)]

            def buf(self, ref, at, n):
                return ref.at[self.slot, :, cols(at, n)]

            def wide(self, ref, at, n):
                return self.buf(ref, at, n)[...].astype(jnp.float32)

            def copy(self, kind, src, dst=None, dev=to_y):
                return rc(kind, self.slot, src, src if dst is None else dst, dev)

            def send(self, kind, dev, src, dst=None):
                self.copy(kind, src, dst, dev).start()

            def got(self, kind, ref):
                self.copy(kind, ref).wait_recv()

            def gone(self, kind, ref):
                self.copy(kind, ref).wait_send()

            def residual(self):
                return pltpu.make_async_copy(x.at[self.rows, cols(mine + t1(yy, s), BOTH)], self.buf(res, 0, BOTH), rssem.at[self.slot])

            def keep(self):
                return pltpu.make_async_copy(self.buf(fin, 0, BOTH), self.y(t1(yy, s), BOTH), lsem.at[self.slot])

        low = jnp.bfloat16

        def grow(e, at, n, more):
            own = e.term(at, n)
            own[...] = own[...] + more

        @stage(0, "mid")
        def _(e):
            for p in range(2):
                e.buf(bb, p * e.wb, e.wb)[...] = e.term(t1(yo, p), e.wb)[...].astype(low)

        @stage(1, "mid")
        def _(e):
            e.gone(BB, e.buf(bb, 0, 2 * e.wb))
            for p in range(2):
                e.buf(sy1, p * e.wa, e.wa)[...] = e.term(t1(yo, p) + e.wb, e.wa)[...].astype(low)

        @stage(1, "end")
        def _(e):
            e.got(BB, e.buf(bb, 0, 2 * e.wb))
            for p in range(2):
                e.buf(sy1, p * e.w1, e.wb)[...] = (e.term(t1(yo, p), e.wb)[...] + e.wide(bb, p * e.wb, e.wb)).astype(low)
                e.buf(sy1, p * e.w1 + e.wb, e.wa)[...] = e.term(t1(yo, p) + e.wb, e.wa)[...].astype(low)
            for q in range(4):
                e.buf(be2, q * e.w2, e.w2)[...] = e.term(e.t2(0, q), e.w2)[...].astype(low)

        @stage(2, "mid")
        def _(e):
            e.gone(Y1, e.buf(sy1, 0, 2 * e.wa))
            e.got(Y1, e.buf(ry1, 0, 2 * e.wa))
            e.got(E2, e.buf(be2, 0, 4 * e.w2))
            for p in range(2):
                grow(e, t1(yy, p) + e.wb, e.wa, e.wide(ry1, p * e.wa, e.wa))
            for r in range(2):
                e.buf(sx2, r * e.w2, e.w2)[...] = (e.term(e.t2(r, so), e.w2)[...] + e.wide(be2, (2 * r + so) * e.w2, e.w2)).astype(low)
                grow(e, e.t2(r, s), e.w2, e.wide(be2, (2 * r + s) * e.w2, e.w2))

        @stage(2, "end")
        def _(e):
            e.gone(Y1, e.buf(sy1, 0, 2 * e.w1))
            e.got(Y1, e.buf(ry1, 0, 2 * e.w1))
            e.gone(E2, e.buf(be2, 0, 4 * e.w2))
            for p in range(2):
                e.buf(be1, p * e.w1, e.w1)[...] = (e.term(t1(yy, p), e.w1)[...] + e.wide(ry1, p * e.w1, e.w1)).astype(low)

        @stage(3, "end")
        def _(e):
            e.gone(E1, e.buf(be1, 0, 2 * e.w1))

        @stage(3, "mid")
        def _(e):
            e.gone(X2, e.buf(sx2, 0, 2 * e.w2))
            e.got(E1, e.buf(be1, 0, 2 * e.w1))
            e.buf(sx1, 0, e.w1)[...] = (e.term(t1(yy, so), e.w1)[...] + e.wide(be1, so * e.w1, e.w1)).astype(low)
            grow(e, t1(yy, s), e.w1, e.wide(be1, s * e.w1, e.w1))
            e.got(X2, e.buf(rx2, 0, 2 * e.w2))
            e.buf(sy2, 0, e.w2)[...] = (e.term(e.t2(yo, s), e.w2)[...] + e.wide(rx2, yo * e.w2, e.w2)).astype(low)
            grow(e, e.t2(yy, s), e.w2, e.wide(rx2, yy * e.w2, e.w2))

        @stage(4, "mid")
        def _(e):
            e.gone(X1, e.buf(sx1, 0, e.w1))
            e.gone(Y2, e.buf(sy2, 0, e.w2))
            e.residual().wait()
            e.got(X1, e.buf(rx1, 0, e.w1))
            e.got(Y2, e.buf(ry2, 0, e.w2))
            for at, n, ref in ((0, e.w1, rx1), (e.w1, e.w2, ry2)):
                e.buf(fin, at, n)[...] = (e.term(t1(yy, s) + at, n)[...] + e.wide(ref, 0, n) + e.wide(res, at, n)).astype(low)

        @stage(5, "mid")
        def _(e):
            for kind in (FP, FX, FY):
                e.gone(kind, e.buf(fin, 0, BOTH))
            e.keep().wait()
            e.got(FX, e.y(t1(yy, so), BOTH))
            e.got(FY, e.y(t1(yo, s), BOTH))

        @stage(5, "end")
        def _(e):
            e.got(FP, e.y(t1(yy, s), BOTH))

        @stage(6, "mid")
        def _(e):
            e.gone(AP, e.y(0, BOTH))
            e.gone(AY, e.y(0, e.w1))
            e.last_hop(lambda: e.gone(CP, e.y(0, e.w2)), lambda: None)
            e.gone(CX, e.y(0, e.w2))
            e.got(AY, e.y(t1(yo, so), e.w1))
            e.got(CX, e.y(e.t2(yo, so), e.w2))

        @stage(6, "end")
        def _(e):
            e.got(AP, e.y(t1(yy, so), BOTH))

            def by_z():
                e.gone(EY0, e.y(0, e.w1))
                e.got(CP, e.y(e.t2(yo, s), e.w2))
                e.got(EY0, e.y(t1(yo, s), e.w1))

            def by_y():
                e.gone(EY0, e.y(0, BOTH))
                e.got(EY0, e.y(t1(yo, s), BOTH))

            e.last_hop(by_z, by_y)

        @stage(7, "end")
        def _(e):
            e.gone(EY1, e.y(0, BOTH))
            e.got(EY1, e.y(t1(yo, so), BOTH))

        @stage(8)
        def _(e):
            e.gone(SIB, e.y(0, HALF))
            e.got(SIB, e.y(0, HALF, other))

        emit()

        def spend():
            greet(lambda n, dev: pl.semaphore_wait(credit.at[n], 1))

        if opens:
            spend() if full else pl.when(m >= LAG)(spend)

        @stage(0, "mid")
        def _(e):
            e.send(BB, to_p, e.buf(bb, 0, 2 * e.wb))

        @stage(1, "end")
        def _(e):
            e.send(Y1, to_y, e.buf(sy1, 0, 2 * e.w1), e.buf(ry1, 0, 2 * e.w1))
            e.send(E2, to_p, e.buf(be2, 0, 4 * e.w2))

        @stage(1, "mid")
        def _(e):
            e.send(Y1, to_y, e.buf(sy1, 0, 2 * e.wa), e.buf(ry1, 0, 2 * e.wa))

        @stage(2, "end")
        def _(e):
            e.send(E1, to_p, e.buf(be1, 0, 2 * e.w1))

        @stage(2, "mid")
        def _(e):
            e.send(X2, to_x, e.buf(sx2, 0, 2 * e.w2), e.buf(rx2, 0, 2 * e.w2))

        @stage(3, "mid")
        def _(e):
            e.send(X1, to_x, e.buf(sx1, 0, e.w1), e.buf(rx1, 0, e.w1))
            e.send(Y2, to_y, e.buf(sy2, 0, e.w2), e.buf(ry2, 0, e.w2))
            e.residual().start()

        @stage(4, "mid")
        def _(e):
            for kind, dev in ((FP, to_p), (FX, to_x), (FY, to_y)):
                e.send(kind, dev, e.buf(fin, 0, BOTH), e.y(t1(yy, s), BOTH))
            e.keep().start()

        @stage(5, "mid")
        def _(e):
            e.send(AP, to_p, e.y(t1(yy, so), BOTH))
            e.send(CX, to_x, e.y(e.t2(yo, s), e.w2))
            e.send(AY, to_y, e.y(t1(yy, so), e.w1))
            e.last_hop(lambda: e.send(CP, to_p, e.y(e.t2(yo, s), e.w2)), lambda: None)

        @stage(5, "end")
        def _(e):
            e.last_hop(*(functools.partial(e.send, EY0, to_y, e.y(t1(yy, s), n)) for n in (e.w1, BOTH)))

        @stage(6, "end")
        def _(e):
            e.send(EY1, to_y, e.y(t1(yy, so), BOTH))

        @stage(7)
        def _(e):
            e.send(SIB, to_s, e.y(0, HALF))

        emit()
        if closes:
            greet(lambda n, dev: signal(credit.at[n], dev))

    wo_sent = rc(WO, 0, wo.at[:, cols(other, HALF)], wos, to_s)

    def out_cols(n):
        n = jnp.where(n == 1, FIRST, jnp.where((n > 1) & (n <= FIRST), n - 1, n))
        return lax.rem(n + 2 * FIRST * yo, HALF // TN) * TN

    def tiles(g):
        u, k = lax.rem(g, UNITS), lax.rem(g, NS)

        def proj(ref, n):
            @pl.when((u >= n * (UQ // 3)) & (u < (n + 1) * (UQ // 3)))
            def _():
                v = u - n * (UQ // 3)
                pltpu.make_async_copy(ref.at[pl.ds(pl.multiple_of(lax.rem(v, QK) * KS, KS), KS), cols(v // QK * TN, TN)], w.at[k], wsem.at[k]).start()

        @pl.when(g < NCH * UNITS)
        def _():
            for n, ref in enumerate((wq, wk, wv)):
                proj(ref, n)

            @pl.when(u >= UQ)
            def _():
                @pl.when(g == UQ)
                def _():
                    wo_sent.wait_recv()

                for ref, at, row in ((wo, mine, 0), (wos, 0, MINE)):
                    src = ref.at[:, cols(at + out_cols(u - UQ), TN)]
                    pltpu.make_async_copy(src, w.at[k, pl.ds(row, MINE)], wsem.at[k]).start()

    def tile(g):
        k = lax.rem(g, NS)
        pltpu.make_async_copy(w.at[k], w.at[k], wsem.at[k]).wait()
        return w.at[k]

    def rows_of(c):
        return pl.ds(pl.multiple_of(c * CH, CH), CH)

    own_rows, other_rows = (pl.ds(pl.multiple_of(k * (CH // 2), CH // 2), CH // 2) for k in (core, 1 - core))

    def fetch(c):
        rows = pl.ds(pl.multiple_of(c * CH + core * (CH // 2), CH // 2), CH // 2)
        return pltpu.make_async_copy(x.at[rows], a.at[own_rows], xsem.at[0])

    def first_rows(n):
        rows = pl.ds(n * (CH // 4), CH // 4)
        return pltpu.make_async_copy(x.at[rows], a.at[rows], xsem.at[n])

    def angles(c):
        place = c * CH + lax.broadcasted_iota(jnp.int32, (CH, HEAD), 0)
        angle = place.astype(jnp.float32) * freq[...]
        first = lax.broadcasted_iota(jnp.int32, (CH, HEAD), 1) < HEAD // 2
        sin = jnp.sin(angle)
        csv[:, :HEAD] = jnp.cos(angle)
        csv[:, HEAD:] = jnp.where(first, -sin, sin)

    def norm(first, last):
        def group(r, _):
            rows = pl.ds(pl.multiple_of(r * TALL, TALL), TALL)
            total = jnp.zeros((TALL, HEAD), jnp.float32)
            for n in range(D // WIDE):
                wide = a[rows, n * WIDE:(n + 1) * WIDE].astype(jnp.float32)
                sq = wide * wide
                for i in range(WIDE // HEAD):
                    total = total + sq[:, i * HEAD:(i + 1) * HEAD]
            scale = lax.rsqrt(jnp.sum(total, -1, keepdims=True) * (1 / D) + 1e-6)
            for n in range(D // WIDE):
                at = slice(n * WIDE, (n + 1) * WIDE)
                a[rows, at] = (a[rows, at].astype(jnp.float32) * scale * jnp.concatenate([gain8[:, at]] * (TALL // 8))).astype(jnp.bfloat16)
            return None

        lax.fori_loop(first // TALL, last // TALL, group, None)

    def turn(b):
        b = b.astype(jnp.float32)
        return (b * csv[:, :HEAD] + pltpu.roll(b, HEAD // 2, 1) * csv[:, HEAD:]).astype(jnp.bfloat16)

    def project(c, u, _):
        g = c * UNITS + u
        ref = tile(g)
        ks, n = lax.rem(u, QK), u // QK
        acc[...] += jnp.dot(a[:, cols(ks * KS, KS)], ref[...], preferred_element_type=jnp.float32)
        tiles(g + NS)

        @pl.when(ks == QK - 1)
        def _():
            heads = [(lax.rem(n, PART) * (TN // HEAD) + i, slice(i * HEAD, (i + 1) * HEAD)) for i in range(TN // HEAD)]

            @pl.when(n < PART)
            def _():
                for h, at in heads:
                    q_s[h] = turn(acc[:, at].astype(jnp.bfloat16))

            @pl.when((n >= PART) & (n < 2 * PART))
            def _():
                for h, at in heads:
                    k_s[h, rows_of(c), :] = turn(acc[:, at].astype(jnp.bfloat16))

            @pl.when(n >= 2 * PART)
            def _():
                for h, at in heads:
                    v_s[h, :, cols(c * CH, CH)] = acc[:, at].astype(jnp.bfloat16).T

            acc[...] = jnp.zeros_like(acc)
        return None

    def attend(c, h0, count):
        e = HEAD**-0.5 * LOG2E
        for i in range(count):
            top_s[i:i + 1, :] = jnp.full((1, CH), NEG, jnp.float32)
            mix_s[i] = jnp.zeros((HEAD + 8, CH), jnp.float32)
        ones = jnp.ones((8, CH), jnp.bfloat16)

        def block(j, masked):
            here = pl.ds(pl.multiple_of(j * CH, CH), CH)
            scores = [_dot(k_s[h0 + i, here, :], q_s[h0 + i], 1, 1) for i in range(count)]
            if masked:
                ok = lax.broadcasted_iota(jnp.int32, (CH, CH), 1) >= lax.broadcasted_iota(jnp.int32, (CH, CH), 0)
            weights, keeps = [], []
            for i, sc in enumerate(scores):
                if masked:
                    sc = jnp.where(ok, sc, -jnp.inf)
                old = top_s[i:i + 1, :]
                top = jnp.maximum(old, sc.max(axis=0, keepdims=True))
                top_s[i:i + 1, :] = top
                weights.append(jnp.exp2((sc - top) * e).astype(jnp.bfloat16))
                keeps.append(jnp.exp2((old - top) * e))
            for i, (p, kp) in enumerate(zip(weights, keeps)):
                values = jnp.concatenate([v_s[h0 + i, :, here], ones], axis=0)
                mix_s[i] = mix_s[i] * kp + _dot(values, p, 1, 0)

        lax.fori_loop(0, c, lambda j, _: block(j, False), None)
        block(c, True)
        for i in range(count):
            out = mix_s[i, :HEAD, :] * (1 / mix_s[i, HEAD:HEAD + 1, :])
            seen[:, cols((h0 + i) * HEAD, HEAD)] = out.T.astype(jnp.bfloat16)

    def out_tile(c, v, _):
        g = c * UNITS + UQ + v
        ref = tile(g)
        term[lax.rem(c, 2), :, cols(out_cols(v), TN)] = jnp.dot(seen[...], ref[...], preferred_element_type=jnp.float32)
        tiles(g + NS)
        return None

    norm_sent = rc(NORM, 0, a.at[own_rows], a.at[own_rows], to_s)
    norm_got = rc(NORM, 0, a.at[other_rows], a.at[other_rows], to_s)
    seen_sent = rc(SEEN, 0, seen.at[:, pl.ds(0, 1024)], seen.at[:, pl.ds(1024, 1024)], to_s)

    if compute:
        for n in range(4):
            first_rows(n).start()
        acc[...] = jnp.zeros_like(acc)
        gain8[...] = jnp.broadcast_to(gain[...].astype(jnp.float32).reshape(1, D), gain8.shape)

        def piece(n, _):
            first_rows(n).wait()

            @pl.when(n == 1)
            def _():
                for g in range(NS):
                    tiles(g)

            norm(n * (CH // 4), (n + 1) * (CH // 4))
            return None

        lax.fori_loop(0, 4, piece, None)

    @pl.when(mid)
    def _():
        pl.semaphore_wait(bar, 4)

    @pl.when(end)
    def _():
        pl.semaphore_wait(bar, 3)

    if compute:
        wo_sent.start()

    def step(n, _):
        c, i = n // PER, lax.rem(n, PER)
        if compute:
            @pl.when((c < NCH) & (i == OUT))
            def _():
                seen_sent.start()

        if comm:
            m = (c - 1) * PER + i + EARLY
            full = m >= LAG * STAGES
            for odd in range(2):
                now = (m >= 0) & (lax.rem(m + LAG, 2) == odd)
                pl.when(now & full)(functools.partial(exchange, m, odd, True))
                pl.when(now & jnp.logical_not(full))(functools.partial(exchange, m, odd))

        def slot(first, last):
            return pl.when((c < NCH) & (i >= first) & (i < last))

        if compute:
            @slot(0, 1)
            def _():
                angles(c)

                @pl.when(c > 0)
                def _():
                    norm_got.wait_recv()
                    norm_sent.wait_send()

            @slot(0, ATT)
            def _():
                lax.fori_loop(i * UQ // ATT, (i + 1) * UQ // ATT, functools.partial(project, c), None)

            @slot(ATT, ATT + 1)
            def _():
                @pl.when(c < NCH - 1)
                def _():
                    fetch(c + 1).start()

            @slot(ATT, OUT)
            def _():
                attend(c, (i - ATT) * (8 // (OUT - ATT)), 8 // (OUT - ATT))

            @slot(OUT, OUT + 1)
            def _():
                @pl.when(c < NCH - 1)
                def _():
                    fetch(c + 1).wait()
                    norm(core * (CH // 2), (core + 1) * (CH // 2))

                seen_sent.wait_recv()
                seen_sent.wait_send()

                @pl.when(c < NCH - 1)
                def _():
                    norm_sent.start()

                out_tile(c, 0, None)

            @slot(OUT + 1, PER)
            def _():
                k, n = i - OUT - 1, PER - OUT - 1
                lax.fori_loop(1 + k * (UO - 1) // n, 1 + (k + 1) * (UO - 1) // n, functools.partial(out_tile, c), None)

        return None

    def final(n, _):
        for odd in range(2):
            m = LATE + 2 * n + odd
            exchange(m, odd, closes=False)
            exchange(m, odd, half=0, opens=False, closes=False)
            exchange(m, odd, half=1, opens=False)
        return None

    lax.fori_loop(0, NCH * PER, step, None)
    if comm:
        lax.fori_loop(0, (NSUB + FAST * STAGES // 2 - LATE) // 2, final, None)
    if comm:
        greet(lambda n, dev: pl.semaphore_wait(credit.at[n], LAG))
    if compute:
        wo_sent.wait_send()


def call(x, gain, freq, wq, wk, wv, wo, compute=True, comm=True, cid=0):
    any_, vmem = pl.BlockSpec(memory_space=pl.ANY), pl.BlockSpec(memory_space=pltpu.VMEM)
    low = jnp.bfloat16
    v, f32 = pltpu.VMEM, jnp.float32
    msg = lambda n: v((KEEP, SUB, n), low)
    return pl.pallas_call(
        functools.partial(kernel, compute=compute, comm=comm),
        out_shape=[jax.ShapeDtypeStruct((ROWS, D), low), jax.ShapeDtypeStruct((1024, HALF), low)],
        in_specs=[any_, vmem, vmem] + [any_] * 4,
        out_specs=[any_, any_],
        scratch_shapes=[
            v((CH, D), low), v((NS, KS, TN), low), v((CH, TN), f32), v((CH, 2 * HEAD), f32), v((8, D), f32),
            v((8, CH, HEAD), low), v((8, ROWS, HEAD), low), v((8, HEAD, ROWS), low), v((CH, 2048), low),
            v((8, CH), f32), v((4, HEAD + 8, CH), f32), v((2, CH, HALF), f32),
            *map(msg, (2 * MB, 4 * M2, 2 * M1, 2 * M1, 2 * M1, 2 * M2, 2 * M2, M1, M1, M2, M2, BOTH, BOTH)),
            pltpu.SemaphoreType.DMA((len(KINDS), KEEP)), pltpu.SemaphoreType.DMA((len(KINDS), KEEP)), pltpu.SemaphoreType.DMA((NS,)),
            pltpu.SemaphoreType.DMA((KEEP,)), pltpu.SemaphoreType.DMA((KEEP,)), pltpu.SemaphoreType.DMA((4,)),
            pltpu.SemaphoreType.REGULAR((4,)),
        ],
        compiler_params=pltpu.CompilerParams(collective_id=cid, has_side_effects=True, vmem_limit_bytes=67043328),
        cost_estimate=pl.CostEstimate(flops=2 * ROWS * D * 4096, transcendentals=8 * ROWS * ROWS, bytes_accessed=2**30),
    )(x, gain, freq, wq, wk, wv, wo)


def solution(mesh, compute=True, comm=True):
    def step(x, gain, wq, wk, wv, wo):
        half = HEAD // 2
        freq = THETA ** (-jnp.arange(half, dtype=jnp.float32) / half)
        y, _ = call(x, gain, jnp.concatenate([freq, freq])[None], wq, wk, wv, wo, compute=compute, comm=comm)
        return y

    tokens, columns = P("dp", None), P(None, "tp")
    return jax.shard_map(step, mesh=mesh, in_specs=(tokens, P(None), columns, columns, columns, P("tp", None)), out_specs=tokens, check_vma=False)
```
